32 devices in a mesh: fsdp: 16 (over z, x, core), tp: 2 (over y).
Axes of the slice: x: 2, y: 2, z: 4, core: 2. Of those that a mesh axis runs over, the one named last changes fastest.
Arguments:
- inputs: bfloat16 [32768, 1024], P(('fsdp', 'tp')), may hold values from -6 to 6
- cotangent: bfloat16 [32768, 1024], P(('fsdp', 'tp')), may hold values from -18 to 18
- first_gain: float32 [1024], replicated, may hold values from 0.5 to 1.5
- first_shift: float32 [1024], replicated, may hold values from -1.5 to 1.5
- second_gain: float32 [1024], replicated, may hold values from 0.5 to 1.5
- second_shift: float32 [1024], replicated, may hold values from -1.5 to 1.5
- project_weight: bfloat16 [1024, 3, 1024], P('fsdp', None, 'tp'), may hold values from -0.1875 to 0.1875
- project_bias: float32 [3, 1024], P(None, 'tp'), may hold values from -1.5 to 1.5
- dense_weight: bfloat16 [1024, 1024], P('tp', 'fsdp'), may hold values from -4 to 4
- dense_bias: float32 [1024], replicated, may hold values from -1.5 to 1.5
- expand_weight: bfloat16 [1024, 4096], P('fsdp', 'tp'), may hold values from -0.1875 to 0.1875
- expand_bias: float32 [4096], P('tp'), may hold values from -2.5 to 2.5
- shrink_weight: bfloat16 [4096, 1024], P('tp', 'fsdp'), may hold values from -0.09375 to 0.09375
- shrink_bias: float32 [1024], replicated, may hold values from -1.5 to 1.5
Outputs:
- output: bfloat16 [32768, 1024], P(('fsdp', 'tp'))
- input_grad: float32 [32768, 1024], P(('fsdp', 'tp'))
- first_gain_grad: float32 [1024], replicated
- first_shift_grad: float32 [1024], replicated
- second_gain_grad: float32 [1024], replicated
- second_shift_grad: float32 [1024], replicated
- project_weight_grad: float32 [1024, 3, 1024], P('fsdp', None, 'tp')
- project_bias_grad: float32 [3, 1024], P(None, 'tp')
- dense_weight_grad: float32 [1024, 1024], P('tp', 'fsdp')
- dense_bias_grad: float32 [1024], replicated
- expand_weight_grad: float32 [1024, 4096], P('fsdp', 'tp')
- expand_bias_grad: float32 [4096], P('tp')
- shrink_weight_grad: float32 [4096, 1024], P('tp', 'fsdp')
- shrink_bias_grad: float32 [1024], replicated
The draws below stay inside these ranges and needn't reach their ends.
All inputs are finite; a program needn't handle non-finite values.
Results may differ from the reference program's by a relative error of at most 0.0094.
Values may be sent and summed in bfloat16 or wider, within the bound.
A program may use at most 320 MiB of HBM per device.

```python
import jax
import jax.numpy as jnp
from jax import lax

D = 1024
H = 16
HS = 64
ROT = 16
FF = 4096
LEN = 2048
TOKENS = 32768


def draw_cotangent(key, part):
    position = jnp.arange(TOKENS).astype(jnp.float32) / TOKENS
    rising = 3.0 ** position
    base = jnp.clip(jax.random.normal(key, (TOKENS, D), jnp.float32), -6.0, 6.0)
    return (base * rising[:, None]).astype(jnp.bfloat16)


def steps_of(stream_key, extent, shards, least, top_value):
    gain, own = 1.0, jax.random.fold_in(stream_key, 6)
    for dim, blocks in shards:
        steps = jnp.exp(jax.random.uniform(jax.random.fold_in(own, dim), (blocks,), jnp.float32, least / len(shards), top_value / len(shards)))
        gain = gain * jnp.repeat(steps, extent[dim] // blocks).reshape([-1 if axis == dim else 1 for axis in range(len(extent))])
    return gain


def scatter_about(stream_key, extent, scale, most, split=(), held_as=jnp.bfloat16):
    factor_of = steps_of(stream_key, extent, split, -0.22, 0.18) if split else 1.0
    values = jax.random.normal(stream_key, extent, jnp.float32) * scale * factor_of
    return jnp.minimum(jnp.maximum(values, -most), most).astype(held_as)


def setup_inputs(seed: int = 0) -> dict:
    arg_keys = jax.random.split(jax.random.key(seed), 15)
    inputs = scatter_about(arg_keys[0], (TOKENS, D), 1.0, 6.0, ((0, 32),))
    cotangent = draw_cotangent(jax.random.fold_in(arg_keys[14], 71), 0)
    first_gain = jnp.clip(1.0 + 0.1 * jax.random.normal(arg_keys[2], (D,), jnp.float32), 0.5, 1.5)
    first_shift = scatter_about(arg_keys[3], (D,), 0.3, 1.5, (), jnp.float32)
    second_gain = jnp.clip(1.0 + 0.1 * jax.random.normal(arg_keys[4], (D,), jnp.float32), 0.5, 1.5)
    second_shift = scatter_about(arg_keys[5], (D,), 0.3, 1.5, (), jnp.float32)
    project_weight = scatter_about(arg_keys[6], (D, 3, D), D ** -0.5, 0.1875, ((0, 16), (2, 2)))
    project_bias = scatter_about(arg_keys[7], (3, D), 0.3, 1.5, ((1, 2),), jnp.float32)
    dense_weight = scatter_about(arg_keys[8], (D, D), (D * 4 // LEN) ** -0.5, 4.0, ((0, 2), (1, 16)))
    dense_bias = scatter_about(arg_keys[9], (D,), 0.3, 1.5, (), jnp.float32)
    expand_weight = scatter_about(arg_keys[10], (D, FF), D ** -0.5, 0.1875, ((0, 16), (1, 2)))
    expand_bias = scatter_about(arg_keys[11], (FF,), 0.5, 2.5, ((0, 2),), jnp.float32)
    shrink_weight = scatter_about(arg_keys[12], (FF, D), FF ** -0.5, 0.09375, ((0, 2), (1, 16)))
    shrink_bias = scatter_about(arg_keys[13], (D,), 0.3, 1.5, (), jnp.float32)
    return dict(inputs=inputs, cotangent=cotangent, first_gain=first_gain, first_shift=first_shift, second_gain=second_gain, second_shift=second_shift, project_weight=project_weight, project_bias=project_bias, dense_weight=dense_weight, dense_bias=dense_bias, expand_weight=expand_weight, expand_bias=expand_bias, shrink_weight=shrink_weight, shrink_bias=shrink_bias)


EPS = 1e-05
HIGHEST = lax.Precision.HIGHEST

@jax.custom_vjp
def low(v):
    return lax.optimization_barrier(v.astype(jnp.bfloat16)).astype(jnp.float32)

@jax.custom_vjp
def low_back(v):
    return v

def low_keep(v):
    return (low(v), None)

def low_pass(kept, grad):
    return (grad,)

def back_keep(v):
    return (v, None)

def back_low(kept, grad):
    return (low(grad),)
low.defvjp(low_keep, low_pass)
low_back.defvjp(back_keep, back_low)

def normalize(values, gain_vector, shift_vector):
    mean_row = lax.optimization_barrier(jnp.mean(values, axis=-1, keepdims=True))
    centred = values - mean_row
    spread = lax.rsqrt(lax.optimization_barrier(jnp.mean(centred * centred, axis=-1, keepdims=True)) + EPS)
    return centred * spread * gain_vector + shift_vector

def rotary_tables(row_count):
    half_rot = ROT // 2
    position = (jnp.arange(row_count) % LEN).astype(jnp.float32)
    inverse = 10000.0 ** (-(jnp.arange(half_rot).astype(jnp.float32) * 2.0) / ROT)
    angle = position[:, None] * inverse[None, :]
    return (jnp.cos(angle), jnp.sin(angle))

def rotate(heads_in, cosine_table, sine_table):
    half_rot = ROT // 2
    first_half = heads_in[..., :half_rot]
    second_half = heads_in[..., half_rot:ROT]
    cos_wide = cosine_table[:, None, :]
    sin_wide = sine_table[:, None, :]
    return jnp.concatenate([first_half * cos_wide - second_half * sin_wide, second_half * cos_wide + first_half * sin_wide, heads_in[..., ROT:]], axis=-1)

def forward(values, first_gain, first_shift, second_gain, second_shift, project_weight, project_bias, dense_weight, dense_bias, expand_weight, expand_bias, shrink_weight, shrink_bias):
    row_count = values.shape[0]
    first_normed = low(normalize(values, first_gain, first_shift))
    second_normed = low(normalize(values, second_gain, second_shift))
    joined_rows = jnp.dot(first_normed, project_weight.reshape(D, 3 * D), precision=HIGHEST, preferred_element_type=jnp.float32).reshape(row_count, 3, D) + project_bias[None]
    joined_rows = low_back(joined_rows)
    cosine_table, sine_table = rotary_tables(row_count)
    queries = low(rotate(joined_rows[:, 0].reshape(row_count, H, HS), cosine_table, sine_table))
    keys_all = low(rotate(joined_rows[:, 1].reshape(row_count, H, HS), cosine_table, sine_table))
    values_all = low(joined_rows[:, 2].reshape(row_count, H, HS))
    raw_scores = jnp.einsum('qhd,khd->hqk', queries, keys_all, precision=HIGHEST) * HS ** (-0.5)
    raw_scores = low_back(raw_scores)
    positions = jnp.arange(row_count)
    causal = positions[None, :] <= positions[:, None]
    scores = jnp.where(causal[None], raw_scores, -1e+30)
    row_top = lax.optimization_barrier(jnp.max(scores, axis=-1, keepdims=True))
    shifted = jnp.exp(scores - row_top)
    attention = low(shifted / lax.optimization_barrier(jnp.sum(shifted, axis=-1, keepdims=True)))
    context = jnp.einsum('hqk,khd->qhd', attention, values_all, precision=HIGHEST).reshape(row_count, D)
    context = low(low_back(context))
    pre_act = low_back(jnp.dot(second_normed, expand_weight, precision=HIGHEST, preferred_element_type=jnp.float32) + expand_bias)
    activation = low(jax.nn.gelu(pre_act, approximate=False))
    branch = jnp.dot(context, dense_weight, precision=HIGHEST, preferred_element_type=jnp.float32) + jnp.dot(activation, shrink_weight, precision=HIGHEST, preferred_element_type=jnp.float32)
    branch = low_back(branch)
    return values + branch + dense_bias + shrink_bias

def add_pair(left_tree, right_tree):
    return left_tree + right_tree

def reference(inputs, cotangent, first_gain, first_shift, second_gain, second_shift, project_weight, project_bias, dense_weight, dense_bias, expand_weight, expand_bias, shrink_weight, shrink_bias):
    params = (first_gain.astype(jnp.float32), first_shift.astype(jnp.float32), second_gain.astype(jnp.float32), second_shift.astype(jnp.float32), project_weight.astype(jnp.float32), project_bias.astype(jnp.float32), dense_weight.astype(jnp.float32), dense_bias.astype(jnp.float32), expand_weight.astype(jnp.float32), expand_bias.astype(jnp.float32), shrink_weight.astype(jnp.float32), shrink_bias.astype(jnp.float32))
    seq_total = TOKENS // LEN
    rows_all = inputs.astype(jnp.float32).reshape(seq_total, LEN, D)
    grads_all = cotangent.astype(jnp.float32).reshape(seq_total, LEN, D)

    def one_sequence(carry, pack):
        seq_rows, seq_grads = pack
        result, backward = jax.vjp(forward, seq_rows, *params)
        found = backward(seq_grads)
        carry = jax.tree.map(add_pair, carry, tuple(found[1:]))
        return (carry, (result.astype(jnp.bfloat16), found[0]))
    zero_tree = tuple((jnp.zeros(item.shape, jnp.float32) for item in params))
    totals, (results, input_grads) = lax.scan(one_sequence, zero_tree, (rows_all, grads_all))
    return (results.reshape(TOKENS, D), input_grads.reshape(TOKENS, D), totals[0], totals[1], totals[2], totals[3], totals[4], totals[5], totals[6], totals[7], totals[8], totals[9], totals[10], totals[11])
```

```python
import functools

import jax
import jax.numpy as jnp
from jax import lax
from jax.experimental import pallas as pl
from jax.experimental.pallas import tpu as pltpu
from jax.sharding import PartitionSpec as P

f32, bf16 = jnp.float32, jnp.bfloat16
HS = 64
ROT = 16
LEN = 2048
EPS = 1e-05
NEG = -1e30
VMEM_LIMIT = 60 << 20
ERFC = (
    0.22567586308569043,
    0.22566953354787173,
    0.20784372127485384,
    0.1685348386069925,
    0.14145750936579315,
    -0.005660950942278366,
    0.16914715407444447,
    -0.18293900460081808,
    0.050271460956987875,
)


def dot(a, b, ca=1, cb=0):
    return lax.dot_general(a, b, (((ca,), (cb,)), ((), ())), preferred_element_type=f32)


def gelu_parts(x):
    t = pl.reciprocal(1.0 + (0.4 * 0.5**0.5) * jnp.abs(x))
    poly = jnp.full_like(t, ERFC[-1])
    for c in ERFC[-2::-1]:
        poly = poly * t + c
    e = jnp.exp(-0.5 * (x * x))
    tail = (0.5 * t) * poly * e
    cdf = jnp.where(x < 0, tail, 1.0 - tail)
    return x * cdf, cdf + x * (e * 0.3989422804014327)


def params():
    return pltpu.CompilerParams(vmem_limit_bytes=VMEM_LIMIT)


def held(rows, cols, col_block=0):
    return pl.BlockSpec((rows, cols), lambda *i: (0, col_block), pipeline_mode=pl.Buffered(1))


def shape(rows, cols, dtype):
    return jax.ShapeDtypeStruct((rows, cols), dtype)


def qkv_kernel(shift, x_ref, vec_ref, w_ref, b_ref, c_ref, sa_ref, sb_ref, n1_ref, n2_ref, st_ref, q_ref, k_ref, v_ref):
    x = x_ref[...].astype(f32)
    mean = jnp.mean(x, axis=1, keepdims=True)
    centred = x - mean
    rstd = lax.rsqrt(jnp.mean(centred * centred, axis=1, keepdims=True) + EPS)
    normal = centred * rstd
    st_ref[:, 0:1] = mean
    st_ref[:, 1:2] = rstd
    n1 = (normal * vec_ref[0:1, :] + vec_ref[1:2, :]).astype(bf16)
    n1_ref[...] = n1
    n2_ref[...] = (normal * vec_ref[2:3, :] + vec_ref[3:4, :]).astype(bf16)
    width = q_ref.shape[1]
    tables = [jnp.concatenate([r[...]] * (width // 128), axis=1) for r in (c_ref, sa_ref, sb_ref)]
    for part, ref in enumerate((q_ref, k_ref, v_ref)):
        y = dot(n1, w_ref[:, part * width : (part + 1) * width]) + b_ref[part : part + 1, :]
        if part < 2:
            y = turn(y, *tables)
        if part == 0:
            y = y * HS**-0.5
        ref[...] = y.astype(bf16)


def turn(y, cos, sin_up, sin_down):
    width = y.shape[1]
    half = ROT // 2
    return y * cos + pltpu.roll(y, width - half, 1) * sin_up + pltpu.roll(y, half, 1) * sin_down


def qkv_call(shift, x, vec, w1, bias, tables, width, rows=256):
    g, d = x.shape
    n = g // rows
    own = lambda c: pl.BlockSpec((rows, c), lambda i, s: (i, 0))
    seq = lambda c: pl.BlockSpec((rows, c), lambda i, s: ((i + s[0] // rows) % n, 0))
    table = pl.BlockSpec((rows, 128), lambda i, s: (((i + s[0] // rows) % n) % (LEN // rows), 0))
    return pl.pallas_call(
        qkv_kernel,
        grid_spec=pltpu.PrefetchScalarGridSpec(
            num_scalar_prefetch=1,
            grid=(n,),
            in_specs=[own(d), held(4, d), held(d, 3 * width), held(3, width), table, table, table],
            out_specs=[own(d), own(d), own(2), seq(width), seq(width), seq(width)],
        ),
        out_shape=[shape(g, d, bf16), shape(g, d, bf16), shape(g, 2, f32)] + [shape(g, width, bf16)] * 3,
        compiler_params=params(),
    )(shift, x, vec, w1, bias, *tables)


def context_grad_kernel(shift, g_ref, w_ref, do_ref):
    do_ref[...] = dot(g_ref[...], w_ref[...]).astype(bf16)


def context_grad_call(shift, grads, w1, width, rows=512):
    g, d = grads.shape
    n = g // rows
    return pl.pallas_call(
        context_grad_kernel,
        grid_spec=pltpu.PrefetchScalarGridSpec(
            num_scalar_prefetch=1,
            grid=(n,),
            in_specs=[pl.BlockSpec((rows, d), lambda i, s: (i, 0)), held(d, width, 3)],
            out_specs=pl.BlockSpec((rows, width), lambda i, s: ((i + s[0] // rows) % n, 0)),
        ),
        out_shape=shape(g, width, bf16),
        compiler_params=params(),
    )(shift, grads, w1)


def attention_kernel(q_ref, k_ref, v_ref, do_ref, c_ref, sa_ref, sb_ref, o_ref, dq_ref, dk_ref, dv_ref, dk_sum, dv_sum, *, block):
    step = pl.program_id(2)
    count = LEN // block
    heads = q_ref.shape[1] // HS

    @pl.when(step == 0)
    def _():
        dk_sum[...] = jnp.zeros_like(dk_sum)
        dv_sum[...] = jnp.zeros_like(dv_sum)

    def turn_back(y, rows):
        return turn(y, c_ref[rows, :], -sa_ref[rows, :], -sb_ref[rows, :])

    def run(i):
        outs, dqs = [], []
        for h in range(heads):
            lanes = slice(h * HS, (h + 1) * HS)
            q, do = q_ref[:, lanes], do_ref[:, lanes]
            parts = [slice(j * block, (j + 1) * block) for j in range(i + 1)]
            scores = [dot(k_ref[rows, lanes], q, 1, 1) for rows in parts]
            key_pos = lax.broadcasted_iota(jnp.int32, (block, block), 0)
            query_pos = lax.broadcasted_iota(jnp.int32, (block, block), 1)
            scores[i] = jnp.where(key_pos <= query_pos, scores[i], NEG)
            top = functools.reduce(jnp.maximum, [jnp.max(s, axis=0, keepdims=True) for s in scores])
            weights = [jnp.exp(s - top) for s in scores]
            total = functools.reduce(jnp.add, [jnp.sum(w, axis=0, keepdims=True) for w in weights])
            scale = 1.0 / total
            weights = [w * scale for w in weights]
            low = [w.astype(bf16) for w in weights]
            mixed = functools.reduce(jnp.add, [dot(v_ref[rows, lanes], low[j], 0, 0) for j, rows in enumerate(parts)])
            do_t = do.astype(f32).T
            delta = jnp.sum(mixed * do_t, axis=0, keepdims=True)
            do_t = do_t.astype(bf16)
            q_t = q.astype(f32).T.astype(bf16)
            dq = 0.0
            for j, rows in enumerate(parts):
                prob_grad = dot(v_ref[rows, lanes], do, 1, 1)
                score_grad = (weights[j] * (prob_grad - delta)).astype(bf16)
                dv_sum[lanes, rows] += dot(do_t, low[j], 1, 1)
                dk_sum[lanes, rows] += dot(q_t, score_grad, 1, 1)
                dq = dq + dot(k_ref[rows, lanes], score_grad, 0, 0)
            outs.append(mixed.T)
            dqs.append(dq.T)
        o_ref[...] = jnp.concatenate(outs, axis=1).astype(bf16)
        here = slice(i * block, (i + 1) * block)
        dq_ref[...] = turn_back(jnp.concatenate(dqs, axis=1) * HS**-0.5, here).astype(bf16)

    for i in range(count):
        pl.when(step == i)(functools.partial(run, i))

    @pl.when(step == count - 1)
    def _():
        for i in range(count):
            rows = slice(i * block, (i + 1) * block)
            dk_ref[rows, :] = turn_back(dk_sum[:, rows].T, rows).astype(bf16)
            dv_ref[rows, :] = dv_sum[:, rows].T.astype(bf16)


def attention_call(q, k, v, do, tables, block=512):
    g, width = q.shape
    seqs, count, pairs = g // LEN, LEN // block, width // 128
    one = pl.BlockSpec((block, 128), lambda s, h, i: (s * count + i, h))
    whole = pl.BlockSpec((LEN, 128), lambda s, h, i: (s, h))
    table = pl.BlockSpec((LEN, 128), lambda s, h, i: (0, 0))
    return pl.pallas_call(
        functools.partial(attention_kernel, block=block),
        grid=(seqs, pairs, count),
        in_specs=[one, whole, whole, one, table, table, table],
        out_specs=[one, one, whole, whole],
        out_shape=[shape(g, width, bf16)] * 4,
        scratch_shapes=[pltpu.VMEM((128, LEN), f32), pltpu.VMEM((128, LEN), f32)],
        compiler_params=params(),
    )(q, k, v, do, *tables)


def first(i):
    return pl.program_id(0) == 0 if i == 0 else pl.program_id(0) == pl.num_programs(0) - 1


def normal_of(x_ref, st_ref):
    return (x_ref[...].astype(f32) - st_ref[:, 0:1]) * st_ref[:, 1:2]


def project_back_kernel(shift, dq_ref, dk_ref, dv_ref, ctx_ref, n1_ref, x_ref, st_ref, g_ref, vec_ref, w_ref, s_ref, dw_ref, cols_ref, bias_ref, acc):
    @pl.when(first(0))
    def _():
        acc[...] = jnp.zeros_like(acc)
        cols_ref[...] = jnp.zeros_like(cols_ref)
        bias_ref[...] = jnp.zeros_like(bias_ref)

    n1 = n1_ref[...]
    width = dq_ref.shape[1]
    s = 0.0
    for part, ref in enumerate((dq_ref, dk_ref, dv_ref)):
        lanes = slice(part * width, (part + 1) * width)
        joined = ref[...]
        bias_ref[part : part + 1, :] += jnp.sum(joined.astype(f32), axis=0, keepdims=True)
        s = s + dot(joined, w_ref[:, lanes], 1, 1)
        acc[:, lanes] += dot(n1, joined, 0, 0)
    acc[:, 3 * width :] += dot(g_ref[...], ctx_ref[...], 0, 0)
    normal = normal_of(x_ref, st_ref)
    cols_ref[0:1, :] += jnp.sum(s * normal, axis=0, keepdims=True)
    cols_ref[1:2, :] += jnp.sum(s, axis=0, keepdims=True)
    s_ref[...] = s * vec_ref[0:1, :]

    @pl.when(first(1))
    def _():
        dw_ref[...] = acc[...].astype(bf16)


def project_back_call(shift, dq, dk, dv, ctx, n1, x, st, grads, vec, w1, rows=256):
    g, d = x.shape
    width = dq.shape[1]
    n = g // rows
    own = lambda c: pl.BlockSpec((rows, c), lambda i, s: (i, 0))
    seq = lambda c: pl.BlockSpec((rows, c), lambda i, s: ((i + s[0] // rows) % n, 0))
    return pl.pallas_call(
        project_back_kernel,
        grid_spec=pltpu.PrefetchScalarGridSpec(
            num_scalar_prefetch=1,
            grid=(n,),
            in_specs=[seq(width)] * 4 + [own(d), own(d), own(2), own(d), held(4, d), held(d, 3 * width)],
            out_specs=[own(d), held(d, 4 * width), held(2, d), held(3, width)],
            scratch_shapes=[pltpu.VMEM((d, 4 * width), f32)],
        ),
        out_shape=[shape(g, d, f32), shape(d, 4 * width, bf16), shape(2, d, f32), shape(3, width, f32)],
        compiler_params=params(),
    )(shift, dq, dk, dv, ctx, n1, x, st, grads, vec, w1)


def feed_forward_kernel(shift, n2_ref, g_ref, ctx_ref, we_ref, ws_ref, wd_ref, be_ref, gp_ref, br_ref, dw_ref, acc, *, chunk):
    @pl.when(first(0))
    def _():
        acc[...] = jnp.zeros_like(acc)

    n2, g = n2_ref[...], g_ref[...]
    branch = dot(ctx_ref[...], wd_ref[...], 1, 1)
    for c in range(we_ref.shape[1] // chunk):
        lanes = slice(c * chunk, (c + 1) * chunk)
        act, slope = gelu_parts(dot(n2, we_ref[:, lanes]) + be_ref[:, lanes])
        act = act.astype(bf16)
        gp_ref[:, lanes] = slope.astype(bf16)
        branch = branch + dot(act, ws_ref[:, lanes], 1, 1)
        acc[:, lanes] += dot(g, act, 0, 0)
    br_ref[...] = branch.astype(bf16)

    @pl.when(first(1))
    def _():
        dw_ref[...] = acc[...].astype(bf16)


def feed_forward_call(shift, n2, grads, ctx, w2, w1, be, rows=512):
    g, d = n2.shape
    hidden, width = w2.shape[1] // 2, ctx.shape[1]
    n = g // rows
    own = lambda c: pl.BlockSpec((rows, c), lambda i, s: (i, 0))
    seq = lambda c: pl.BlockSpec((rows, c), lambda i, s: ((i + s[0] // rows) % n, 0))
    return pl.pallas_call(
        functools.partial(feed_forward_kernel, chunk=min(hidden, 2048)),
        grid_spec=pltpu.PrefetchScalarGridSpec(
            num_scalar_prefetch=1,
            grid=(n,),
            in_specs=[own(d), own(d), seq(width), held(d, hidden, 0), held(d, hidden, 1), held(d, width, 3), held(1, hidden)],
            out_specs=[own(hidden), own(d), held(d, hidden)],
            scratch_shapes=[pltpu.VMEM((d, hidden), f32)],
        ),
        out_shape=[shape(g, hidden, bf16), shape(g, d, bf16), shape(d, hidden, bf16)],
        compiler_params=params(),
    )(shift, n2, grads, ctx, w2, w2, w1, be)


def feed_back_kernel(n2_ref, g_ref, gp_ref, s1_ref, x_ref, st_ref, vec_ref, we_ref, ws_ref, s_ref, dw_ref, cols_ref, bias_ref, acc, *, chunk):
    @pl.when(first(0))
    def _():
        acc[...] = jnp.zeros_like(acc)
        cols_ref[...] = jnp.zeros_like(cols_ref)
        bias_ref[...] = jnp.zeros_like(bias_ref)

    n2, g = n2_ref[...], g_ref[...]
    s = 0.0
    for c in range(we_ref.shape[1] // chunk):
        lanes = slice(c * chunk, (c + 1) * chunk)
        pre_grad = (dot(g, ws_ref[:, lanes]) * gp_ref[:, lanes].astype(f32)).astype(bf16)
        bias_ref[:, lanes] += jnp.sum(pre_grad.astype(f32), axis=0, keepdims=True)
        s = s + dot(pre_grad, we_ref[:, lanes], 1, 1)
        acc[:, lanes] += dot(n2, pre_grad, 0, 0)
    normal = normal_of(x_ref, st_ref)
    cols_ref[0:1, :] += jnp.sum(s * normal, axis=0, keepdims=True)
    cols_ref[1:2, :] += jnp.sum(s, axis=0, keepdims=True)
    s_ref[...] = (s1_ref[...] + s * vec_ref[2:3, :]).astype(bf16)

    @pl.when(first(1))
    def _():
        dw_ref[...] = acc[...].astype(bf16)


def feed_back_call(n2, grads, gp, s1, x, st, vec, w2, rows=256):
    g, d = n2.shape
    hidden = gp.shape[1]
    own = lambda c: pl.BlockSpec((rows, c), lambda i: (i, 0))
    return pl.pallas_call(
        functools.partial(feed_back_kernel, chunk=min(hidden, 1024)),
        grid=(g // rows,),
        in_specs=[own(d), own(d), own(hidden), own(d), own(d), own(2), held(4, d), held(d, hidden, 0), held(d, hidden, 1)],
        out_specs=[own(d), held(d, hidden), held(2, d), held(1, hidden)],
        out_shape=[shape(g, d, bf16), shape(d, hidden, bf16), shape(2, d, f32), shape(1, hidden, f32)],
        scratch_shapes=[pltpu.VMEM((d, hidden), f32)],
        compiler_params=params(),
    )(n2, grads, gp, s1, x, st, vec, w2, w2)


def rotary_tables():
    half = ROT // 2
    position = jnp.arange(LEN).astype(f32)
    inverse = 10000.0 ** (-(jnp.arange(half).astype(f32) * 2.0) / ROT)
    angle = position[:, None] * inverse[None, :]
    cos, sin = jnp.cos(angle), jnp.sin(angle)
    rest = jnp.zeros((LEN, HS - ROT), f32)
    none = jnp.zeros((LEN, half), f32)
    pair = lambda *a: jnp.tile(jnp.concatenate(a, axis=1), (1, 128 // HS))
    return pair(cos, cos, rest + 1.0), pair(-sin, none, rest), pair(none, sin, rest)


def make_body(tp):
    def swap(a):
        return lax.ppermute(a, "tp", [(0, 1), (1, 0)])

    def body(inputs, cotangent, first_gain, first_shift, second_gain, second_shift, project_weight, project_bias, dense_weight, dense_bias, expand_weight, expand_bias, shrink_weight, shrink_bias):
        rows, d = inputs.shape
        width = dense_weight.shape[0]
        hidden = shrink_weight.shape[0]
        part = project_weight.shape[0]
        me = lax.axis_index("tp")
        if tp == 2:
            shift = (me * rows).astype(jnp.int32)[None]
            gather_rows = lambda a: jnp.concatenate([a, swap(a)], axis=0)
            scatter_rows = lambda a: a[:rows].astype(f32) + swap(a[rows:]).astype(f32)
        else:
            shift = jnp.zeros((1,), jnp.int32)
            gather_rows = lambda a: lax.all_gather(a, "tp", axis=0, tiled=True)
            scatter_rows = lambda a: lax.psum_scatter(a, "tp", scatter_dimension=0, tiled=True).astype(f32)
        shard1 = jnp.concatenate([project_weight.reshape(part, 3 * width), dense_weight.T], axis=1)
        shard2 = jnp.concatenate([expand_weight, shrink_weight.T], axis=1)
        w1 = lax.all_gather(shard1, "fsdp", axis=0, tiled=True)
        x = gather_rows(inputs)
        w2 = lax.all_gather(shard2, "fsdp", axis=0, tiled=True)
        grads = gather_rows(cotangent)
        vec = jnp.stack([first_gain, first_shift, second_gain, second_shift])
        tables = rotary_tables()
        n1, n2, st, q, k, v = qkv_call(shift, x, vec, w1, project_bias, tables, width)
        do = context_grad_call(shift, grads, w1, width)
        ctx, dq, dk, dv = attention_call(q, k, v, do, tables)
        s1, dw1, cols1, bias1 = project_back_call(shift, dq, dk, dv, ctx, n1, x, st, grads, vec, w1)
        dw1 = lax.psum_scatter(dw1, "fsdp", scatter_dimension=0, tiled=True).astype(f32)
        gp, branch, dws = feed_forward_call(shift, n2, grads, ctx, w2, w1, expand_bias[None])
        branch = scatter_rows(branch)
        s, dwe, cols2, bias2 = feed_back_call(n2, grads, gp, s1, x, st, vec, w2)
        s = scatter_rows(s)
        dw2 = lax.psum_scatter(jnp.concatenate([dwe, dws], axis=1), "fsdp", scatter_dimension=0, tiled=True).astype(f32)
        own_rows, own_grads = inputs.astype(f32), cotangent.astype(f32)
        output = (own_rows + branch + dense_bias + shrink_bias).astype(bf16)
        own_st = st[:rows] if tp == 2 else lax.dynamic_slice_in_dim(st, me * rows, rows, 0)
        normal = (own_rows - own_st[:, 0:1]) * own_st[:, 1:2]
        term = own_st[:, 1:2] * (s - jnp.mean(s, axis=1, keepdims=True) - normal * jnp.mean(s * normal, axis=1, keepdims=True))
        input_grad = own_grads + term
        local = jnp.concatenate([bias1.reshape(-1), bias2.reshape(-1)])
        slots = lax.dynamic_update_slice_in_dim(jnp.zeros((tp, local.shape[0]), f32), local[None], me, 0)
        small = jnp.concatenate([cols1.reshape(-1), cols2.reshape(-1), jnp.sum(own_grads, axis=0), slots.reshape(-1)])
        small = lax.psum(small, ("fsdp", "tp"))
        cols = small[: 5 * d].reshape(5, d)
        local = lax.dynamic_slice_in_dim(small[5 * d :].reshape(tp, -1), me, 1, 0)[0]
        return (
            output,
            input_grad,
            cols[0],
            cols[1],
            cols[2],
            cols[3],
            dw1[:, : 3 * width].reshape(part, 3, width),
            local[: 3 * width].reshape(3, width),
            dw1[:, 3 * width :].T,
            cols[4],
            dw2[:, :hidden],
            local[3 * width :],
            dw2[:, hidden:].T,
            cols[4],
        )

    return body


def solution(mesh):
    rows, rep = P(("fsdp", "tp"), None), P()
    return jax.shard_map(
        make_body(mesh.shape["tp"]),
        mesh=mesh,
        in_specs=(rows, rows, rep, rep, rep, rep, P("fsdp", None, "tp"), P(None, "tp"), P("tp", "fsdp"), rep, P("fsdp", "tp"), P("tp"), P("tp", "fsdp"), rep),
        out_specs=(rows, rows, rep, rep, rep, rep, P("fsdp", None, "tp"), P(None, "tp"), P("tp", "fsdp"), rep, P("fsdp", "tp"), P("tp"), P("tp", "fsdp"), rep),
        check_vma=False,
    )
```

```python
import functools

import jax
import jax.numpy as jnp
from jax import lax
from jax.experimental import pallas as pl
from jax.experimental.pallas import tpu as pltpu
from jax.sharding import PartitionSpec as P

f32, bf16 = jnp.float32, jnp.bfloat16
HS = 64
ROT = 16
LEN = 2048
EPS = 1e-05
NEG = -1e30
VMEM_LIMIT = 60 << 20
PIECES = 2
ERFC = (
    0.22567586308569043,
    0.22566953354787173,
    0.20784372127485384,
    0.1685348386069925,
    0.14145750936579315,
    -0.005660950942278366,
    0.16914715407444447,
    -0.18293900460081808,
    0.050271460956987875,
)


def dot(a, b, ca=1, cb=0):
    return lax.dot_general(a, b, (((ca,), (cb,)), ((), ())), preferred_element_type=f32)


def gelu_parts(x):
    t = pl.reciprocal(1.0 + (0.4 * 0.5**0.5) * jnp.abs(x))
    poly = jnp.full_like(t, ERFC[-1])
    for c in ERFC[-2::-1]:
        poly = poly * t + c
    e = jnp.exp(-0.5 * (x * x))
    tail = (0.5 * t) * poly * e
    cdf = jnp.where(x < 0, tail, 1.0 - tail)
    return x * cdf, cdf + x * (e * 0.3989422804014327)


def call(kernel, grid, in_specs, out_specs, out_shape, scratch, flops, scalars=1, collective=None):
    size = lambda a: a.dtype.itemsize * a.size
    return lambda *args: pl.pallas_call(
        kernel,
        grid_spec=pltpu.PrefetchScalarGridSpec(num_scalar_prefetch=scalars, grid=grid, in_specs=in_specs, out_specs=out_specs, scratch_shapes=scratch),
        out_shape=out_shape,
        compiler_params=pltpu.CompilerParams(vmem_limit_bytes=VMEM_LIMIT, collective_id=collective, has_side_effects=collective is not None),
        cost_estimate=pl.CostEstimate(flops=int(flops), transcendentals=0, bytes_accessed=sum(map(size, args)) + sum(map(size, out_shape))),
    )(*args)


def held(rows, cols, col_block=0):
    return pl.BlockSpec((rows, cols), lambda *i: (0, col_block), pipeline_mode=pl.Buffered(1))


def shape(rows, cols, dtype):
    return jax.ShapeDtypeStruct((rows, cols), dtype)


def both(rows, cols, count):
    return [
        pl.BlockSpec((rows, cols), lambda i, *s: (jnp.minimum(i, count - 1), 0)),
        pl.BlockSpec((rows, cols), lambda i, *s: (jnp.maximum(i - count, 0), 0)),
    ]


def own_order(rows, cols):
    return pl.BlockSpec((rows, cols), lambda i, *s: (i, 0))


def seq_order(rows, cols, n):
    return pl.BlockSpec((rows, cols), lambda i, shift, *s: ((i + shift[0] // rows) % n, 0))


def pick(refs, count):
    return jnp.where(pl.program_id(0) < count, refs[0][...], refs[1][...])


def put(refs, count, value):
    for ref, here in zip(refs, (pl.program_id(0) < count, pl.program_id(0) >= count)):

        @pl.when(here)
        def _():
            ref[...] = value


def at_first():
    return pl.when(pl.program_id(0) == 0)


def at_last():
    return pl.when(pl.program_id(0) == pl.num_programs(0) - 1)


def block_order(j):
    f = lax.axis_index("fsdp")
    z, x, core = lax.div(f, 4), lax.rem(lax.div(f, 2), 2), lax.rem(f, 2)
    other_core, other_x, k = 1 - j // 8, 1 - j // 4 % 2, j % 4
    x = 1 - x if other_x else x
    core = 1 - core if other_core else core
    return lax.rem(z + k, 4) * 4 + x * 2 + core


def put_blocks(fsdp, refs, acc):
    size, wide = acc.shape[0] // fsdp, acc.shape[1] // PIECES
    for j in range(fsdp):
        rows = pl.ds(pl.multiple_of(block_order(j) * size, size), size) if fsdp == 16 else slice(j * size, (j + 1) * size)
        at = j % (fsdp // 2) * size
        for p in range(PIECES):
            refs[j // (fsdp // 2)][p, at : at + size, :] = acc[rows, p * wide : (p + 1) * wide].astype(bf16)


def pieces(d, cols):
    dims = (PIECES, d // 2, cols // PIECES)
    return pl.BlockSpec(dims, lambda *i: (0, 0, 0), pipeline_mode=pl.Buffered(1)), jax.ShapeDtypeStruct(dims, bf16)


def neighbours():
    f, t = lax.axis_index("fsdp"), lax.axis_index("tp")
    core, x = lax.rem(f, 2), lax.rem(lax.div(f, 2), 2)
    around = [(lax.rem(f + 4 * k, 16), t) for k in range(1, 4)]
    return {"core": (f + 1 - 2 * core, t), "x": (f + 2 - 4 * x, t), "y": (f, 1 - t), "z": around}


def greet(to):
    barrier = pltpu.get_barrier_semaphore()
    peers = [to["core"], to["x"], to["y"], *to["z"]]
    for peer in peers:
        pl.semaphore_signal(barrier, inc=1, device_id=peer, device_id_type=pl.DeviceIdType.MESH)
    pl.semaphore_wait(barrier, len(peers))


def remote(src, dst, sems, at, peer):
    return pltpu.make_async_remote_copy(
        src_ref=src, dst_ref=dst, send_sem=sems[0].at[at], recv_sem=sems[1].at[at], device_id=peer, device_id_type=pl.DeviceIdType.MESH
    )


def sem_pair(count):
    return [pltpu.SemaphoreType.DMA((count,)), pltpu.SemaphoreType.DMA((count,))]


class Reduce:
    def __init__(self, send, keep, out, scratch, to):
        self.send, self.keep, self.out, self.to = send, keep, out, to
        self.got, self.send2, self.got2, self.send3, self.got3, *sems = scratch
        self.sems = [sems[0:2], sems[2:4], sems[4:6]]

    @staticmethod
    def scratch(d, cols):
        rows, wide = d // 16, cols // PIECES
        buffer = lambda n: pltpu.VMEM((PIECES, n * rows, wide), bf16)
        return [buffer(8), buffer(4), buffer(4), buffer(3), buffer(3)] + sem_pair(PIECES) + sem_pair(PIECES) + sem_pair(3 * PIECES)

    def copy1(self, p):
        return remote(self.send.at[p], self.got.at[p], self.sems[0], p, self.to["core"])

    def copy2(self, p):
        return remote(self.send2.at[p], self.got2.at[p], self.sems[1], p, self.to["x"])

    def copies3(self, p):
        rows = self.out.shape[0]
        cut = lambda ref, k: ref.at[p, k * rows : (k + 1) * rows]
        return [remote(cut(self.send3, k), cut(self.got3, k), self.sems[2], 3 * p + k, self.to["z"][k]) for k in range(3)]

    def begin(self, p):
        self.copy1(p).start()

    def across_x(self, p):
        self.copy1(p).wait()
        rows = slice(0, self.send2.shape[1])
        self.send2[p] = (self.keep[p, rows].astype(f32) + self.got[p, rows].astype(f32)).astype(bf16)
        self.copy2(p).start()

    def along_z(self, p):
        self.copy2(p).wait()
        rows, wide = self.out.shape[0], self.send2.shape[2]
        half = 4 * rows
        for k in (1, 2, 3, 0):
            here = slice(half + k * rows, half + (k + 1) * rows)
            total = self.keep[p, here].astype(f32) + self.got[p, here].astype(f32) + self.got2[p, k * rows : (k + 1) * rows].astype(f32)
            if k:
                self.send3[p, (k - 1) * rows : k * rows] = total.astype(bf16)
            else:
                self.out[:, p * wide : (p + 1) * wide] = total
        for copy in self.copies3(p):
            copy.start()

    def end(self, p):
        rows, wide = self.out.shape[0], self.send2.shape[2]
        for copy in self.copies3(p):
            copy.wait()
        got = [self.got3[p, k * rows : (k + 1) * rows].astype(f32) for k in range(3)]
        self.out[:, p * wide : (p + 1) * wide] += got[0] + got[1] + got[2]


def at_step(i):
    return pl.when(pl.program_id(0) == i)


def turn(y, cos, sin_up, sin_down):
    width = y.shape[1]
    half = ROT // 2
    return y * cos + pltpu.roll(y, width - half, 1) * sin_up + pltpu.roll(y, half, 1) * sin_down


def qkv_kernel(shift, x_ref, y_ref, vec_ref, w_ref, b_ref, c_ref, sa_ref, sb_ref, n1_ref, n2_ref, st_ref, q_ref, k_ref, v_ref, *, count):
    x = pick((x_ref, y_ref), count).astype(f32)
    mean = jnp.mean(x, axis=1, keepdims=True)
    centred = x - mean
    rstd = lax.rsqrt(jnp.mean(centred * centred, axis=1, keepdims=True) + EPS)
    normal = centred * rstd
    st_ref[:, 0:1] = mean
    st_ref[:, 1:2] = rstd
    n1 = (normal * vec_ref[0:1, :] + vec_ref[1:2, :]).astype(bf16)
    n1_ref[...] = n1
    n2_ref[...] = (normal * vec_ref[2:3, :] + vec_ref[3:4, :]).astype(bf16)
    width = q_ref.shape[1]
    tables = [jnp.concatenate([r[...]] * (width // 128), axis=1) for r in (c_ref, sa_ref, sb_ref)]
    for part, ref in enumerate((q_ref, k_ref, v_ref)):
        y = dot(n1, w_ref[:, part * width : (part + 1) * width]) + b_ref[part : part + 1, :]
        if part < 2:
            y = turn(y, *tables)
        if part == 0:
            y = y * HS**-0.5
        ref[...] = y.astype(bf16)


def qkv_call(shift, x, vec, w1, bias, tables, width, rows=256):
    d = x[0].shape[1]
    count = x[0].shape[0] // rows
    n = count + x[1].shape[0] // rows
    g = n * rows
    table = pl.BlockSpec((rows, 128), lambda i, shift: (((i + shift[0] // rows) % n) % (LEN // rows), 0))
    return call(
        functools.partial(qkv_kernel, count=count),
        (n,),
        both(rows, d, count) + [held(4, d), held(d, 3 * width), held(3, width), table, table, table],
        [own_order(rows, d), own_order(rows, d), own_order(rows, 2)] + [seq_order(rows, width, n)] * 3,
        [shape(g, d, bf16), shape(g, d, bf16), shape(g, 2, f32)] + [shape(g, width, bf16)] * 3,
        [],
        6 * g * d * width,
    )(shift, *x, vec, w1, bias, *tables)


def context_grad_kernel(shift, g_ref, w_ref, do_ref):
    do_ref[...] = dot(g_ref[...], w_ref[...]).astype(bf16)


def context_grad_call(shift, grads, w1, width, rows=512):
    g, d = grads.shape
    return call(
        context_grad_kernel,
        (g // rows,),
        [own_order(rows, d), held(d, width, 3)],
        [own_order(rows, width)],
        [shape(g, width, bf16)],
        [],
        2 * g * d * width,
    )(shift, grads, w1)[0]


def attention_kernel(start, *refs, block, opens, closes):
    q_ref, k_ref, v_ref, do_ref, c_ref, sa_ref, sb_ref = refs[:7]
    refs = list(refs[7:])
    before = [] if opens else [refs.pop(0), refs.pop(0)]
    o_ref, dq_ref, dk_ref, dv_ref, dk_sum, dv_sum = refs
    step = pl.program_id(2)
    here = start[0] // block + step
    heads = q_ref.shape[1] // HS

    @pl.when(step == 0)
    def _():
        dk_sum[...] = jnp.zeros_like(dk_sum) if opens else before[0][...]
        dv_sum[...] = jnp.zeros_like(dv_sum) if opens else before[1][...]

    def turn_back(y, rows):
        return turn(y, c_ref[rows, :], -sa_ref[rows, :], -sb_ref[rows, :])

    def run(i):
        outs, dqs = [], []
        for h in range(heads):
            lanes = slice(h * HS, (h + 1) * HS)
            q, do = q_ref[:, lanes], do_ref[:, lanes]
            parts = [slice(j * block, (j + 1) * block) for j in range(i + 1)]
            scores = [dot(k_ref[rows, lanes], q, 1, 1) for rows in parts]
            key_pos = lax.broadcasted_iota(jnp.int32, (block, block), 0)
            query_pos = lax.broadcasted_iota(jnp.int32, (block, block), 1)
            scores[i] = jnp.where(key_pos <= query_pos, scores[i], NEG)
            top = functools.reduce(jnp.maximum, [jnp.max(s, axis=0, keepdims=True) for s in scores])
            weights = [jnp.exp(s - top) for s in scores]
            total = functools.reduce(jnp.add, [jnp.sum(w, axis=0, keepdims=True) for w in weights])
            scale = 1.0 / total
            weights = [w * scale for w in weights]
            low = [w.astype(bf16) for w in weights]
            mixed = functools.reduce(jnp.add, [dot(v_ref[rows, lanes], low[j], 0, 0) for j, rows in enumerate(parts)])
            do_t = do.astype(f32).T
            delta = jnp.sum(mixed * do_t, axis=0, keepdims=True)
            do_t = do_t.astype(bf16)
            q_t = q.astype(f32).T.astype(bf16)
            dq = 0.0
            for j, rows in enumerate(parts):
                prob_grad = dot(v_ref[rows, lanes], do, 1, 1)
                score_grad = (weights[j] * (prob_grad - delta)).astype(bf16)
                dv_sum[lanes, rows] += dot(do_t, low[j], 1, 1)
                dk_sum[lanes, rows] += dot(q_t, score_grad, 1, 1)
                dq = dq + dot(k_ref[rows, lanes], score_grad, 0, 0)
            outs.append(mixed.T)
            dqs.append(dq.T)
        o_ref[...] = jnp.concatenate(outs, axis=1).astype(bf16)
        rows = slice(i * block, (i + 1) * block)
        dq_ref[...] = turn_back(jnp.concatenate(dqs, axis=1) * HS**-0.5, rows).astype(bf16)

    for i in range(LEN // block):
        pl.when(here == i)(functools.partial(run, i))

    @pl.when(step == pl.num_programs(2) - 1)
    def _():
        if not closes:
            dk_ref[...] = dk_sum[...]
            dv_ref[...] = dv_sum[...]
            return
        for i in range(LEN // block):
            rows = slice(i * block, (i + 1) * block)
            dk_ref[rows, :] = turn_back(dk_sum[:, rows].T, rows).astype(bf16)
            dv_ref[rows, :] = dv_sum[:, rows].T.astype(bf16)


def attention_call(start, q, k, v, do, tables, before=None, closes=True, block=512):
    g, width = q.shape
    rows = do.shape[0]
    seqs, pairs = g // LEN, width // 128
    count = rows // seqs // block
    query = pl.BlockSpec((block, 128), lambda s, h, i, start: (s * count + start[0] // block + i, h))
    one = pl.BlockSpec((block, 128), lambda s, h, i, start: (s * count + i, h))
    whole = pl.BlockSpec((LEN, 128), lambda s, h, i, start: (s, h))
    sums = pl.BlockSpec((128, LEN), lambda s, h, i, start: (h, s))
    table = pl.BlockSpec((LEN, 128), lambda s, h, i, start: (0, 0))
    before = before or ()
    return call(
        functools.partial(attention_kernel, block=block, opens=not before, closes=closes),
        (seqs, pairs, count),
        [query, whole, whole, one, table, table, table] + [sums] * len(before),
        [one, one] + [whole if closes else sums] * 2,
        [shape(rows, width, bf16)] * 2 + [shape(g, width, bf16) if closes else shape(width, g, f32)] * 2,
        [pltpu.VMEM((128, LEN), f32), pltpu.VMEM((128, LEN), f32)],
        24 * rows * LEN * width,
    )(start, q, k, v, do, *tables, *before)


def normal_of(refs, st_ref, count):
    return (pick(refs, count).astype(f32) - st_ref[:, 0:1]) * st_ref[:, 1:2]


def project_back_kernel(shift, qo_ref, qt_ref, dk_ref, dv_ref, co_ref, ct_ref, n1_ref, x_ref, y_ref, st_ref, go_ref, gt_ref, vec_ref, w_ref, s_ref, send_ref, keep_ref, cols_ref, bias_ref, acc, *, count, fsdp):
    @at_first()
    def _():
        acc[...] = jnp.zeros_like(acc)
        cols_ref[...] = jnp.zeros_like(cols_ref)
        bias_ref[...] = jnp.zeros_like(bias_ref)

    n1 = n1_ref[...]
    width = dk_ref.shape[1]
    s = 0.0
    for part, joined in enumerate((pick((qo_ref, qt_ref), count), dk_ref[...], dv_ref[...])):
        lanes = slice(part * width, (part + 1) * width)
        bias_ref[part : part + 1, :] += jnp.sum(joined.astype(f32), axis=0, keepdims=True)
        s = s + dot(joined, w_ref[:, lanes], 1, 1)
        acc[:, lanes] += dot(n1, joined, 0, 0)
    acc[:, 3 * width :] += dot(pick((go_ref, gt_ref), count), pick((co_ref, ct_ref), count), 0, 0)
    normal = normal_of((x_ref, y_ref), st_ref, count)
    cols_ref[0:1, :] += jnp.sum(s * normal, axis=0, keepdims=True)
    cols_ref[1:2, :] += jnp.sum(s, axis=0, keepdims=True)
    s_ref[...] = s * vec_ref[0:1, :]

    @at_last()
    def _():
        put_blocks(fsdp, (send_ref, keep_ref), acc)


def project_back_call(shift, fsdp, dq, dk, dv, ctx, n1, x, st, grads, vec, w1, rows=256):
    g, d = n1.shape
    width = dk.shape[1]
    n, count = g // rows, x[0].shape[0] // rows
    return call(
        functools.partial(project_back_kernel, count=count, fsdp=fsdp),
        (n,),
        both(rows, width, count)
        + [seq_order(rows, width, n)] * 2
        + both(rows, width, count)
        + [own_order(rows, d)]
        + both(rows, d, count)
        + [own_order(rows, 2)]
        + both(rows, d, count)
        + [held(4, d), held(d, 3 * width)],
        [own_order(rows, d), *[pieces(d, 4 * width)[0]] * 2, held(2, d), held(3, width)],
        [shape(g, d, f32), *[pieces(d, 4 * width)[1]] * 2, shape(2, d, f32), shape(3, width, f32)],
        [pltpu.VMEM((d, 4 * width), f32)],
        14 * g * d * width,
    )(shift, *dq, dk, dv, *ctx, n1, *x, st, *grads, vec, w1)


def feed_forward_kernel(n2_ref, go_ref, gt_ref, co_ref, ct_ref, we_ref, ws_ref, wd_ref, be_ref, *refs, count, fsdp, fast):
    if fast:
        x_ref, bias_ref, d_send, d_keep, gp_ref, out_ref, send_ref, keep_ref, dw1_ref, acc, to_owner, from_other, *scratch = refs
        to = neighbours()
        reduce = Reduce(d_send, d_keep, dw1_ref, scratch[2:], to)
        row_copy = lambda b: remote(to_owner.at[b], from_other.at[b], scratch[:2], b, to["y"])
    else:
        gp_ref, out_ref, others_ref, send_ref, keep_ref, acc = refs
    step = pl.program_id(0)

    @at_first()
    def _():
        acc[...] = jnp.zeros_like(acc)
        if fast:
            greet(to)
            for p in range(PIECES):
                reduce.begin(p)

    if fast:
        for at, what in ((1, "x"), (3, 0), (5, 1), (7, "end")):

            @at_step(at)
            def _():
                for p in range(PIECES) if what in ("x", "end") else [what]:
                    {"x": reduce.across_x, "end": reduce.end}.get(what, reduce.along_z)(p)

        for b in range(count):

            @at_step(b + 1)
            def _():
                row_copy(b).start()

    own = step >= count
    n2, g = n2_ref[...], jnp.where(own, go_ref[...], gt_ref[...])
    branch = dot(jnp.where(own, co_ref[...], ct_ref[...]), wd_ref[...], 1, 1)
    act, slope = gelu_parts(dot(n2, we_ref[...]) + be_ref[...])
    act = act.astype(bf16)
    gp_ref[...] = slope.astype(bf16)
    branch = branch + dot(act, ws_ref[...], 1, 1)
    acc[...] += dot(g, act, 0, 0)
    if fast:

        @pl.when(jnp.logical_not(own))
        def _():
            to_owner[step] = branch.astype(bf16)

        for b in range(count):

            @at_step(b + count)
            def _():
                row_copy(b).wait()
                out_ref[...] = (x_ref[...].astype(f32) + (branch + from_other[b].astype(f32)) + bias_ref[...]).astype(bf16)

    else:
        put((others_ref, out_ref), count, branch.astype(bf16))

    @at_last()
    def _():
        put_blocks(fsdp, (send_ref, keep_ref), acc)


def feed_forward_call(fsdp, n2, grads, ctx, w2, w1, be, more=None, rows=256):
    g, d = n2.shape
    hidden, width = w2.shape[1] // 2, ctx[0].shape[1]
    own = grads[0].shape[0]
    n = g // rows
    count = own // rows if more else (g - own) // rows
    first = lambda c: pl.BlockSpec((rows, c), lambda i, *s: (jnp.minimum(i, count - 1), 0))
    second = lambda c: pl.BlockSpec((rows, c), lambda i, *s: (jnp.maximum(i - count, 0), 0))
    turned = lambda c: pl.BlockSpec((rows, c), lambda i, *s: ((i + own // rows) % n, 0))
    ins = [turned(d), second(d), first(d), second(width), first(width), held(d, hidden, 0), held(d, hidden, 1), held(d, width, 3), held(1, hidden)]
    half = pieces(d, hidden)
    acc = pltpu.VMEM((d, hidden), f32)
    flops = g * d * (6 * hidden + 2 * width)
    kernel = functools.partial(feed_forward_kernel, count=count, fsdp=fsdp, fast=bool(more))
    args = (n2, *grads, *ctx, w2, w2, w1, be)
    if not more:
        outs = [turned(hidden), second(d), first(d), half[0], half[0]]
        shapes = [shape(g, hidden, bf16), shape(own, d, bf16), shape(g - own, d, bf16), half[1], half[1]]
        return call(kernel, (n,), ins, outs, shapes, [acc], flops, 0)(*args)
    part = d // 16
    ins += [second(d), held(1, d), pl.BlockSpec(memory_space=pl.ANY), pieces(d, 4 * width)[0]]
    outs = [turned(hidden), second(d), half[0], half[0], held(part, 4 * width)]
    shapes = [shape(g, hidden, bf16), shape(own, d, bf16), half[1], half[1], shape(part, 4 * width, f32)]
    rows_buffer = pltpu.VMEM((count, rows, d), bf16)
    scratch = [acc, rows_buffer, rows_buffer] + sem_pair(count) + Reduce.scratch(d, 4 * width)
    return call(kernel, (n,), ins, outs, shapes, scratch, flops, 0, collective=0)(*args, *more)


def feed_back_kernel(n2_ref, go_ref, gt_ref, gp_ref, s1_ref, x_ref, y_ref, st_ref, vec_ref, we_ref, ws_ref, *refs, count, last, fsdp):
    s_refs = refs[: 1 + last]
    send_ref, keep_ref, cols_ref, bias_ref, acc = refs[1 + last :]

    @at_first()
    def _():
        acc[...] = jnp.zeros_like(acc)
        cols_ref[...] = jnp.zeros_like(cols_ref)
        bias_ref[...] = jnp.zeros_like(bias_ref)

    n2, g = n2_ref[...], pick((go_ref, gt_ref), count)
    pre_grad = (dot(g, ws_ref[...]) * gp_ref[...].astype(f32)).astype(bf16)
    bias_ref[...] += jnp.sum(pre_grad.astype(f32), axis=0, keepdims=True)
    s = dot(pre_grad, we_ref[...], 1, 1)
    acc[...] += dot(n2, pre_grad, 0, 0)
    normal = normal_of((x_ref, y_ref), st_ref, count)
    cols_ref[0:1, :] += jnp.sum(s * normal, axis=0, keepdims=True)
    cols_ref[1:2, :] += jnp.sum(s, axis=0, keepdims=True)
    s = s1_ref[...] + s * vec_ref[2:3, :]
    if last:
        put(s_refs, count, s.astype(bf16))
    else:
        s_refs[0][...] = s

    @at_last()
    def _():
        put_blocks(fsdp, (send_ref, keep_ref), acc)


def feed_back_call(fsdp, n2, grads, gp, s1, x, st, vec, w2, half, last, rows=256):
    g, d = n2.shape
    hidden = gp.shape[1] // 2
    own = x[0].shape[0]
    n, count = g // rows, own // rows
    return call(
        functools.partial(feed_back_kernel, count=count, last=last, fsdp=fsdp),
        (n,),
        [own_order(rows, d)]
        + both(rows, d, count)
        + [pl.BlockSpec((rows, hidden), lambda i, *s: (i, half)), own_order(rows, d)]
        + both(rows, d, count)
        + [own_order(rows, 2), held(4, d), held(d, hidden, half), held(d, hidden, 2 + half)],
        (both(rows, d, count) if last else [own_order(rows, d)]) + [pieces(d, hidden)[0]] * 2 + [held(2, d), held(1, hidden)],
        ([shape(own, d, bf16), shape(g - own, d, bf16)] if last else [shape(g, d, f32)])
        + [pieces(d, hidden)[1]] * 2
        + [shape(2, d, f32), shape(1, hidden, f32)],
        [pltpu.VMEM((d, hidden), f32)],
        6 * g * d * hidden,
        0,
    )(n2, *grads, gp, s1, *x, st, vec, w2, w2)


def rotary_tables():
    half = ROT // 2
    position = jnp.arange(LEN).astype(f32)
    inverse = 10000.0 ** (-(jnp.arange(half).astype(f32) * 2.0) / ROT)
    angle = position[:, None] * inverse[None, :]
    cos, sin = jnp.cos(angle), jnp.sin(angle)
    rest = jnp.zeros((LEN, HS - ROT), f32)
    none = jnp.zeros((LEN, half), f32)
    period = lambda *a: jnp.tile(jnp.concatenate(a, axis=1), (1, 128 // HS))
    return period(cos, cos, rest + 1.0), period(-sin, none, rest), period(none, sin, rest)


CORE, X = 1, 2


def flip(a, bit):
    return lax.ppermute(a, "fsdp", [(i, i ^ bit) for i in range(16)])


def along_z(a, k):
    return lax.ppermute(a, "fsdp", [(i, (i + 4 * k) % 16) for i in range(16)])


def reduce_rows(send, keep):
    half = send.shape[1] // 2
    quarter = half // 4
    got = flip(send, CORE)
    add = lambda a, b, rows: (a[:, rows].astype(f32) + b[:, rows].astype(f32)).astype(bf16)
    got2 = flip(add(keep, got, slice(0, half)), X)
    total = lambda k: sum(a[:, half + k * quarter : half + (k + 1) * quarter].astype(f32) for a in (keep, got)) + got2[:, k * quarter : (k + 1) * quarter].astype(f32)
    return join(sum([along_z(total(k).astype(bf16), k).astype(f32) for k in (1, 2, 3)], total(0)))


def join(a):
    return jnp.concatenate(list(a), axis=1)


def sum_all(a, over_all):
    for bit in (1, 2, 4, 8):
        a = a + flip(a, bit)
    head = a[:over_all]
    return jnp.concatenate([head + lax.ppermute(head, "tp", [(0, 1), (1, 0)]), a[over_all:]])


def make_body(fsdp, tp):
    fast = (fsdp, tp) == (16, 2)

    def body(inputs, cotangent, first_gain, first_shift, second_gain, second_shift, project_weight, project_bias, dense_weight, dense_bias, expand_weight, expand_bias, shrink_weight, shrink_bias):
        rows, d = inputs.shape
        width = dense_weight.shape[0]
        hidden = shrink_weight.shape[0]
        part = project_weight.shape[0]
        me = lax.axis_index("tp")
        swap = lambda a: lax.ppermute(a, "tp", [(0, 1), (1, 0)])
        split = lambda a: (a[:rows], a[rows:])
        zero = jnp.zeros((1,), jnp.int32)
        vec = jnp.stack([first_gain, first_shift, second_gain, second_shift])
        shard1 = jnp.concatenate([project_weight.reshape(part, 3 * width), dense_weight.T], axis=1)
        shard2 = jnp.concatenate([expand_weight, shrink_weight.T], axis=1)
        if fast:
            shift = (me * rows).astype(jnp.int32)[None]
            x = (inputs, swap(inputs))
            later, _ = lax.optimization_barrier((cotangent, x[1]))
            grads = (cotangent, swap(later))
        else:
            shift = zero
            x = split(lax.all_gather(inputs, "tp", axis=0, tiled=True))
            grads = split(lax.all_gather(cotangent, "tp", axis=0, tiled=True))
        w1 = lax.all_gather(shard1, "fsdp", axis=0, tiled=True)
        w2 = lax.all_gather(shard2, "fsdp", axis=0, tiled=True)
        tables = rotary_tables()
        n1, n2, st, q, k, v = qkv_call(shift, x, vec, w1, project_bias, tables, width)
        if fast:
            do = context_grad_call(zero, cotangent, w1, width)
            *own, dk, dv = attention_call(shift, q, k, v, do, tables, closes=False)
            late, *_ = lax.optimization_barrier((grads[1], own))
            grads = (cotangent, late)
            do = context_grad_call(zero, late, w1, width)
            *others, dk, dv = attention_call(rows - shift, q, k, v, do, tables, (dk, dv))
            ctx, dq = zip(own, others)
        else:
            do = context_grad_call(zero, jnp.concatenate(grads), w1, width)
            ctx, dq, dk, dv = attention_call(zero, q, k, v, do, tables)
            ctx, dq = split(ctx), split(dq)
        s, *dw1, cols1, bias1 = project_back_call(shift, fsdp, dq, dk, dv, ctx, n1, x, st, grads, vec, w1)
        out_bias = dense_bias + shrink_bias
        if fast:
            gp, output, *dws, dw1 = feed_forward_call(fsdp, n2, grads, ctx, w2, w1, expand_bias[None], (inputs, out_bias[None], *dw1))
        else:
            gp, *branch = feed_forward_call(fsdp, n2, grads, ctx, w2, w1, expand_bias[None])
            branch, dws = branch[:2], branch[2:]
        s, *dwe, cols2, bias2 = feed_back_call(fsdp, n2, grads, gp, s, x, st, vec, w2, 0, False)
        *s, send, keep, cols3, bias3 = feed_back_call(fsdp, n2, grads, gp, s, x, st, vec, w2, 1, True)
        own_rows, own_grads = inputs.astype(f32), cotangent.astype(f32)
        cols = jnp.concatenate([cols1, cols2 + cols3, jnp.sum(own_grads, axis=0, keepdims=True)]).reshape(-1)
        local = jnp.concatenate([bias1.reshape(-1), bias2.reshape(-1), bias3.reshape(-1)])
        if fast:
            s = s[0].astype(f32) + swap(s[1]).astype(f32)
            own_st = st[:rows]
            scatter = lambda pair: reduce_rows(*pair)
            small = sum_all(jnp.concatenate([cols, local]), cols.shape[0])
            cols, local = small[: cols.shape[0]], small[cols.shape[0] :]
        else:
            over = lambda a, axis: lax.psum_scatter(jnp.concatenate(a), axis, scatter_dimension=0, tiled=True).astype(f32)
            s = over(s, "tp")
            output = (own_rows + over(branch, "tp") + out_bias).astype(bf16)
            own_st = lax.dynamic_slice_in_dim(st, me * rows, rows, 0)
            scatter = lambda pair: over([join(a) for a in pair], "fsdp")
            dw1 = scatter(dw1)
            cols = lax.psum(cols, ("fsdp", "tp"))
            local = lax.psum(local, "fsdp")
        cols = cols.reshape(5, d)
        dws, dwe, dwf = scatter(dws), scatter(dwe), scatter((send, keep))
        normal = (own_rows - own_st[:, 0:1]) * own_st[:, 1:2]
        term = own_st[:, 1:2] * (s - jnp.mean(s, axis=1, keepdims=True) - normal * jnp.mean(s * normal, axis=1, keepdims=True))
        return (
            output,
            own_grads + term,
            cols[0],
            cols[1],
            cols[2],
            cols[3],
            dw1[:, : 3 * width].reshape(part, 3, width),
            local[: 3 * width].reshape(3, width),
            dw1[:, 3 * width :].T,
            cols[4],
            jnp.concatenate([dwe, dwf], axis=1),
            local[3 * width :],
            dws.T,
            cols[4],
        )

    return body


def solution(mesh):
    rows, rep = P(("fsdp", "tp"), None), P()
    return jax.shard_map(
        make_body(mesh.shape["fsdp"], mesh.shape["tp"]),
        mesh=mesh,
        in_specs=(rows, rows, rep, rep, rep, rep, P("fsdp", None, "tp"), P(None, "tp"), P("tp", "fsdp"), rep, P("fsdp", "tp"), P("tp"), P("tp", "fsdp"), rep),
        out_specs=(rows, rows, rep, rep, rep, rep, P("fsdp", None, "tp"), P(None, "tp"), P("tp", "fsdp"), rep, P("fsdp", "tp"), P("tp"), P("tp", "fsdp"), rep),
        check_vma=False,
    )
```

```python
import functools

import jax
import jax.numpy as jnp
from jax import lax
from jax.experimental import pallas as pl
from jax.experimental.pallas import tpu as pltpu
from jax.sharding import PartitionSpec as P

f32, bf16 = jnp.float32, jnp.bfloat16
HS = 64
ROT = 16
LEN = 2048
EPS = 1e-05
NEG = -1e30
VMEM_LIMIT = 60 << 20
PIECES = 2
ERFC = (
    0.22567586308569043,
    0.22566953354787173,
    0.20784372127485384,
    0.1685348386069925,
    0.14145750936579315,
    -0.005660950942278366,
    0.16914715407444447,
    -0.18293900460081808,
    0.050271460956987875,
)


def dot(a, b, ca=1, cb=0):
    return lax.dot_general(a, b, (((ca,), (cb,)), ((), ())), preferred_element_type=f32)


def gelu_parts(x):
    t = pl.reciprocal(1.0 + (0.4 * 0.5**0.5) * jnp.abs(x))
    poly = jnp.full_like(t, ERFC[-1])
    for c in ERFC[-2::-1]:
        poly = poly * t + c
    e = jnp.exp(-0.5 * (x * x))
    tail = (0.5 * t) * poly * e
    cdf = jnp.where(x < 0, tail, 1.0 - tail)
    return x * cdf, cdf + x * (e * 0.3989422804014327)


def call(kernel, grid, in_specs, out_specs, out_shape, scratch, flops, scalars=1, collective=None):
    size = lambda a: a.dtype.itemsize * a.size
    return lambda *args: pl.pallas_call(
        kernel,
        grid_spec=pltpu.PrefetchScalarGridSpec(num_scalar_prefetch=scalars, grid=grid, in_specs=in_specs, out_specs=out_specs, scratch_shapes=scratch),
        out_shape=out_shape,
        compiler_params=pltpu.CompilerParams(vmem_limit_bytes=VMEM_LIMIT, collective_id=collective, has_side_effects=collective is not None),
        cost_estimate=pl.CostEstimate(flops=int(flops), transcendentals=0, bytes_accessed=sum(map(size, args)) + sum(map(size, out_shape))),
    )(*args)


def held(rows, cols, col_block=0):
    return pl.BlockSpec((rows, cols), lambda *i: (0, col_block), pipeline_mode=pl.Buffered(1))


def weight_of(w2, p, half=None):
    _, rows, cols = w2.shape
    if half is not None:
        cols = cols // 2
    return pl.BlockSpec((None, rows, cols), lambda *i: (p, 0, half or 0), pipeline_mode=pl.Buffered(1))


def shape(rows, cols, dtype):
    return jax.ShapeDtypeStruct((rows, cols), dtype)


def both(rows, cols, count):
    return [
        pl.BlockSpec((rows, cols), lambda i, *s: (jnp.minimum(i, count - 1), 0)),
        pl.BlockSpec((rows, cols), lambda i, *s: (jnp.maximum(i - count, 0), 0)),
    ]


def own_order(rows, cols):
    return pl.BlockSpec((rows, cols), lambda i, *s: (i, 0))


def seq_order(rows, cols, n):
    return pl.BlockSpec((rows, cols), lambda i, shift, *s: ((i + shift[0] // rows) % n, 0))


def pick(refs, count):
    return jnp.where(pl.program_id(0) < count, refs[0][...], refs[1][...])


def put(refs, count, value):
    for ref, here in zip(refs, (pl.program_id(0) < count, pl.program_id(0) >= count)):

        @pl.when(here)
        def _():
            ref[...] = value


def at_first():
    return pl.when(pl.program_id(0) == 0)


def at_last():
    return pl.when(pl.program_id(0) == pl.num_programs(0) - 1)


def block_order(j):
    f = lax.axis_index("fsdp")
    z, x, core = lax.div(f, 4), lax.rem(lax.div(f, 2), 2), lax.rem(f, 2)
    other_core, other_x, k = 1 - j // 8, 1 - j // 4 % 2, j % 4
    x = 1 - x if other_x else x
    core = 1 - core if other_core else core
    return lax.rem(z + k, 4) * 4 + x * 2 + core


def put_blocks(fsdp, refs, acc):
    size, wide = acc.shape[0] // fsdp, acc.shape[1] // PIECES
    for j in range(fsdp):
        rows = pl.ds(pl.multiple_of(block_order(j) * size, size), size) if fsdp == 16 else slice(j * size, (j + 1) * size)
        at = j % (fsdp // 2) * size
        for p in range(PIECES):
            refs[j // (fsdp // 2)][p, at : at + size, :] = acc[rows, p * wide : (p + 1) * wide].astype(bf16)


def pieces(d, cols):
    dims = (PIECES, d // 2, cols // PIECES)
    return pl.BlockSpec(dims, lambda *i: (0, 0, 0), pipeline_mode=pl.Buffered(1)), jax.ShapeDtypeStruct(dims, bf16)


def neighbours():
    f, t = lax.axis_index("fsdp"), lax.axis_index("tp")
    core, x = lax.rem(f, 2), lax.rem(lax.div(f, 2), 2)
    around = [(lax.rem(f + 4 * k, 16), t) for k in range(1, 4)]
    z_pair = (f + 4 - 8 * lax.rem(lax.div(f, 4), 2), t)
    return {"core": (f + 1 - 2 * core, t), "x": (f + 2 - 4 * x, t), "y": (f, 1 - t), "z": around, "z_pair": z_pair}


def greet(to):
    barrier = pltpu.get_barrier_semaphore()
    peers = [to["core"], to["x"], to["y"], *to["z"]]
    for peer in peers:
        pl.semaphore_signal(barrier, inc=1, device_id=peer, device_id_type=pl.DeviceIdType.MESH)
    pl.semaphore_wait(barrier, len(peers))


def remote(src, dst, sems, at, peer):
    return pltpu.make_async_remote_copy(
        src_ref=src, dst_ref=dst, send_sem=sems[0].at[at], recv_sem=sems[1].at[at], device_id=peer, device_id_type=pl.DeviceIdType.MESH
    )


def sem_pair(count):
    return [pltpu.SemaphoreType.DMA((count,)), pltpu.SemaphoreType.DMA((count,))]


class Reduce:
    def __init__(self, send, keep, out, scratch, to):
        self.send, self.keep, self.out, self.to = send, keep, out, to
        self.got, self.send2, self.got2, self.send3, self.got3, *sems = scratch
        self.sems = [sems[0:2], sems[2:4], sems[4:6]]
        self.count, rows, self.wide = self.got.shape
        self.rows = rows // 8

    @staticmethod
    def scratch(d, cols, count=PIECES):
        rows, wide = d // 16, cols // count
        buffer = lambda n: pltpu.VMEM((count, n * rows, wide), bf16)
        return [buffer(8), buffer(4), buffer(4), buffer(3), buffer(3)] + sem_pair(count) + sem_pair(count) + sem_pair(3 * count)

    def block(self, j):
        return slice(j * self.rows, (j + 1) * self.rows)

    def emit(self, p, total, add=False):
        if len(self.out.shape) == 2:
            self.out[:, self.cols(p)] = total + self.out[:, self.cols(p)] if add else total
            return
        width = self.out.shape[2]
        for r in range(self.wide // width):
            at, here = p * (self.wide // width) + r, total[:, r * width : (r + 1) * width]
            self.out[at] = here + self.out[at] if add else here

    def cols(self, p):
        return slice(p * self.wide, (p + 1) * self.wide)

    def copy1(self, p):
        return remote(self.send.at[p], self.got.at[p], self.sems[0], p, self.to["core"])

    def copy2(self, p):
        return remote(self.send2.at[p], self.got2.at[p], self.sems[1], p, self.to["x"])

    def copies3(self, p):
        cut = lambda ref, k: ref.at[p, self.block(k)]
        return [remote(cut(self.send3, k), cut(self.got3, k), self.sems[2], 3 * p + k, self.to["z"][k]) for k in range(3)]

    def across_core(self, p):
        self.copy1(p).start()

    def across_x(self, p):
        self.copy1(p).wait()
        for j in range(4):
            self.send2[p, self.block(j)] = (self.keep(p, j) + self.got[p, self.block(j)].astype(f32)).astype(bf16)
        self.copy2(p).start()

    def along_z(self, p):
        self.copy2(p).wait()
        for k in (1, 2, 3, 0):
            total = self.keep(p, 4 + k) + self.got[p, self.block(4 + k)].astype(f32) + self.got2[p, self.block(k)].astype(f32)
            if k:
                self.send3[p, self.block(k - 1)] = total.astype(bf16)
            else:
                self.emit(p, total)
        for copy in self.copies3(p):
            copy.start()

    def end(self, p):
        for copy in self.copies3(p):
            copy.wait()
        got = [self.got3[p, self.block(k)].astype(f32) for k in range(3)]
        self.emit(p, got[0] + got[1] + got[2], add=True)


def kept(ref, d):
    rows = d // 16
    return lambda p, j: ref[p, j * rows : (j + 1) * rows].astype(f32)


class SumAll:
    def __init__(self, parts, got, sems, to):
        self.parts, self.got, self.sems = parts, got, sems
        self.peers = [to["core"], to["x"], to["z"][1], to["z_pair"], to["y"]]

    def copy(self, i):
        return remote(self.parts.at[i], self.got.at[i], self.sems, i, self.peers[i])

    def start(self, i):
        self.copy(i).start()

    def turn(self, i):
        self.copy(i).wait()
        self.parts[i + 1] = self.parts[i] + self.got[i]
        self.copy(i + 1).start()

    def end(self, rows_over_tp):
        last = len(self.peers) - 1
        self.copy(last).wait()
        row = lax.broadcasted_iota(jnp.int32, self.parts.shape[1:], 0)
        return self.parts[last] + jnp.where(row < rows_over_tp, self.got[last], 0.0)


def at_step(i):
    return pl.when(pl.program_id(0) == i)


def turn(y, cos, sin_up, sin_down):
    width = y.shape[1]
    half = ROT // 2
    return y * cos + pltpu.roll(y, width - half, 1) * sin_up + pltpu.roll(y, half, 1) * sin_down


def norms(x, vec, n1_ref, n2_ref, st_ref):
    x = x.astype(f32)
    mean = jnp.mean(x, axis=1, keepdims=True)
    centred = x - mean
    rstd = lax.rsqrt(jnp.mean(centred * centred, axis=1, keepdims=True) + EPS)
    normal = centred * rstd
    st_ref[:, 0:1] = mean
    st_ref[:, 1:2] = rstd
    n1 = (normal * vec[0][...] + vec[1][...]).astype(bf16)
    n1_ref[...] = n1
    n2_ref[...] = (normal * vec[2][...] + vec[3][...]).astype(bf16)
    return n1


def project(part, n1, w, b_ref, tables):
    y = dot(n1, w) + b_ref[part : part + 1, :]
    if part < 2:
        y = turn(y, *[jnp.concatenate([t] * (y.shape[1] // 128), axis=1) for t in tables])
    if part == 0:
        y = y * HS**-0.5
    return y.astype(bf16)


def qkv_kernel(shift, x_ref, y_ref, v0_ref, v1_ref, v2_ref, v3_ref, w_ref, b_ref, c_ref, sa_ref, sb_ref, n1_ref, n2_ref, st_ref, q_ref, k_ref, v_ref, *, count):
    n1 = norms(pick((x_ref, y_ref), count), [v0_ref, v1_ref, v2_ref, v3_ref], n1_ref, n2_ref, st_ref)
    width = q_ref.shape[1]
    for part, ref in enumerate((q_ref, k_ref, v_ref)):
        ref[...] = project(part, n1, w_ref[:, part * width : (part + 1) * width], b_ref, [c_ref[...], sa_ref[...], sb_ref[...]])


def qkv_call(shift, x, vec, w1, bias, tables, width, rows=256):
    d = x[0].shape[1]
    count = x[0].shape[0] // rows
    n = count + x[1].shape[0] // rows
    g = n * rows
    table = pl.BlockSpec((rows, 128), lambda i, shift: (((i + shift[0] // rows) % n) % (LEN // rows), 0))
    return call(
        functools.partial(qkv_kernel, count=count),
        (n,),
        both(rows, d, count) + [held(1, d)] * 4 + [held(d, 3 * width), held(3, width), table, table, table],
        [own_order(rows, d), own_order(rows, d), own_order(rows, 2)] + [seq_order(rows, width, n)] * 3,
        [shape(g, d, bf16), shape(g, d, bf16), shape(g, 2, f32)] + [shape(g, width, bf16)] * 3,
        [],
        6 * g * d * width,
    )(shift, *x, *vec, w1, bias, *tables)


def context_grad_kernel(shift, g_ref, w_ref, do_ref):
    do_ref[...] = dot(g_ref[...], w_ref[...]).astype(bf16)


def context_grad_call(shift, grads, w1, width, rows=512):
    g, d = grads.shape
    return call(
        context_grad_kernel,
        (g // rows,),
        [own_order(rows, d), held(d, width, 3)],
        [own_order(rows, width)],
        [shape(g, width, bf16)],
        [],
        2 * g * d * width,
    )(shift, grads, w1)[0]


def attend(i, q_all, do_all, k_ref, v_ref, dk_sum, dv_sum, tables, block):
    outs, dqs = [], []
    parts = [slice(j * block, (j + 1) * block) for j in range(i + 1)]
    for h in range(q_all.shape[1] // HS):
        lanes = slice(h * HS, (h + 1) * HS)
        q, do = q_all[:, lanes], do_all[:, lanes]
        scores = [dot(k_ref[rows, lanes], q, 1, 1) for rows in parts]
        key_pos = lax.broadcasted_iota(jnp.int32, (block, block), 0)
        query_pos = lax.broadcasted_iota(jnp.int32, (block, block), 1)
        scores[i] = jnp.where(key_pos <= query_pos, scores[i], NEG)
        top = functools.reduce(jnp.maximum, [jnp.max(s, axis=0, keepdims=True) for s in scores])
        weights = [jnp.exp(s - top) for s in scores]
        total = functools.reduce(jnp.add, [jnp.sum(w, axis=0, keepdims=True) for w in weights])
        scale = 1.0 / total
        weights = [w * scale for w in weights]
        low = [w.astype(bf16) for w in weights]
        mixed = functools.reduce(jnp.add, [dot(v_ref[rows, lanes], low[j], 0, 0) for j, rows in enumerate(parts)])
        do_t = do.astype(f32).T
        delta = jnp.sum(mixed * do_t, axis=0, keepdims=True)
        do_t = do_t.astype(bf16)
        q_t = q.astype(f32).T.astype(bf16)
        dq = 0.0
        for j, rows in enumerate(parts):
            prob_grad = dot(v_ref[rows, lanes], do, 1, 1)
            score_grad = (weights[j] * (prob_grad - delta)).astype(bf16)
            dv_sum[lanes, rows] += dot(do_t, low[j], 1, 1)
            dk_sum[lanes, rows] += dot(q_t, score_grad, 1, 1)
            dq = dq + dot(k_ref[rows, lanes], score_grad, 0, 0)
        outs.append(mixed.T)
        dqs.append(dq.T)
    dq = turn_back(jnp.concatenate(dqs, axis=1) * HS**-0.5, tables, parts[i])
    return jnp.concatenate(outs, axis=1).astype(bf16), dq.astype(bf16)


def turn_back(y, tables, rows):
    cos, sin_up, sin_down = (t[rows, :] for t in tables)
    return turn(y, cos, -sin_up, -sin_down)


def put_sums(dk_ref, dv_ref, dk_sum, dv_sum, tables, block):
    for i in range(LEN // block):
        rows = slice(i * block, (i + 1) * block)
        dk_ref[rows, :] = turn_back(dk_sum[:, rows].T, tables, rows).astype(bf16)
        dv_ref[rows, :] = dv_sum[:, rows].T.astype(bf16)


def attention_kernel(q_ref, k_ref, v_ref, do_ref, c_ref, sa_ref, sb_ref, o_ref, dq_ref, dk_ref, dv_ref, dk_sum, dv_sum, *, block):
    step = pl.program_id(2)
    tables = (c_ref, sa_ref, sb_ref)

    @pl.when(step == 0)
    def _():
        dk_sum[...] = jnp.zeros_like(dk_sum)
        dv_sum[...] = jnp.zeros_like(dv_sum)

    for i in range(LEN // block):

        @pl.when(step == i)
        def _():
            o_ref[...], dq_ref[...] = attend(i, q_ref[...], do_ref[...], k_ref, v_ref, dk_sum, dv_sum, tables, block)

    @pl.when(step == pl.num_programs(2) - 1)
    def _():
        put_sums(dk_ref, dv_ref, dk_sum, dv_sum, tables, block)


def attention_call(q, k, v, do, tables, block=512):
    g, width = q.shape
    seqs, pairs, count = g // LEN, width // 128, LEN // block
    one = pl.BlockSpec((block, 128), lambda s, h, i: (s * count + i, h))
    whole = pl.BlockSpec((LEN, 128), lambda s, h, i: (s, h))
    return call(
        functools.partial(attention_kernel, block=block),
        (seqs, pairs, count),
        [one, whole, whole, one] + [held(LEN, 128)] * 3,
        [one, one, whole, whole],
        [shape(g, width, bf16)] * 4,
        [pltpu.VMEM((128, LEN), f32), pltpu.VMEM((128, LEN), f32)],
        24 * g * LEN * width,
        0,
    )(q, k, v, do, *tables)


ROWS, BLOCK = 256, 512


INVERSE = [10000.0 ** (-2.0 * j / ROT) for j in range(ROT // 2)]


def put_tables(cos_ref, up_ref, down_ref):
    half = ROT // 2
    lane = lax.rem(lax.broadcasted_iota(jnp.int32, (ROWS, 128), 1), HS)
    inverse = functools.reduce(lambda a, j: jnp.where(lax.rem(lane, half) == j, INVERSE[j], a), range(half), jnp.zeros((ROWS, 128), f32))
    for i in range(LEN // ROWS):
        rows = slice(i * ROWS, (i + 1) * ROWS)
        position = (lax.broadcasted_iota(jnp.int32, (ROWS, 128), 0) + i * ROWS).astype(f32)
        angle = position * inverse
        cos, sin = jnp.cos(angle), jnp.sin(angle)
        cos_ref[rows, :] = jnp.where(lane < ROT, cos, 1.0)
        up_ref[rows, :] = jnp.where(lane < half, -sin, 0.0)
        down_ref[rows, :] = jnp.where(jnp.logical_and(lane >= half, lane < ROT), sin, 0.0)


class Gather:
    def __init__(self, all_ref, piece, sems, to):
        self.all, self.piece, self.to = all_ref, piece, to
        self.sems = [sems[2 * i : 2 * i + 2] for i in range(3)]
        f = lax.axis_index("fsdp")
        self.z, self.x, self.core = lax.div(f, 4), lax.rem(lax.div(f, 2), 2), lax.rem(f, 2)

    @staticmethod
    def scratch(count):
        return sem_pair(3 * count) + sem_pair(count) + sem_pair(count)

    def copies_z(self, p):
        mine = self.all.at[p, self.z, self.x, self.core]
        return [remote(self.piece(p), mine, self.sems[0], 3 * p + k, self.to["z"][k]) for k in range(3)]

    def copy_x(self, p):
        mine = self.all.at[p, :, self.x, self.core]
        return remote(mine, mine, self.sems[1], p, self.to["x"])

    def copy_core(self, p):
        mine = self.all.at[p, :, :, self.core]
        return remote(mine, mine, self.sems[2], p, self.to["core"])

    def along_z(self, p):
        for copy in self.copies_z(p):
            copy.start()

    def across_x(self, p):
        for copy in self.copies_z(p):
            copy.wait()
        self.copy_x(p).start()

    def across_core(self, p):
        self.copy_x(p).wait()
        self.copy_core(p).start()

    def end(self, p):
        self.copy_core(p).wait()


def choose(own, out_ref, own_ref, others):
    @pl.when(own)
    def _():
        out_ref[...] = own_ref[...]

    @pl.when(jnp.logical_not(own))
    def _():
        out_ref[...] = others()


def head_kernel(
    x_ref, x_hbm, g_ref, g_hbm, project_ref, dense_ref, expand_ref, shrink_ref, v0_ref, v1_ref, v2_ref, v3_ref, b_ref,
    n1_ref, n2_ref, st_ref, o_ref, dq_ref, dk_ref, dv_ref, w_ref, x_other, g_other, w2_ref,
    w, x_got, g_got, q_all, k_all, v_all, do_all, dk_sum, dv_sum, c_ref, sa_ref, sb_ref, local_sem, *sems, own, pairs,
):
    step = pl.program_id(0)
    count = own // ROWS
    blocks = own // BLOCK
    n = 2 * count
    t = lax.axis_index("tp")
    to = neighbours()
    tables = (c_ref, sa_ref, sb_ref)
    width = w.shape[-1]
    d = w.shape[1] * w.shape[2] * w.shape[3] * w.shape[4]
    lanes = lambda p: slice(p * width, (p + 1) * width)
    weight = lambda p: w[p].reshape(d, width)
    x_sems, g_sems, sems = sems[0:2], sems[2:4], sems[4:]
    rows_of = lambda ref, i, size: ref.at[pl.ds(i * size, size)]
    x_copy = lambda i: remote(rows_of(x_hbm, i, ROWS), x_got.at[i], x_sems, i, to["y"])
    g_copy = lambda i: remote(rows_of(g_hbm, i, BLOCK), g_got.at[i], g_sems, i, to["y"])
    gather1 = Gather(w, lambda p: dense_ref if p == 3 else project_ref.at[p], sems[:6], to)
    gather2 = Gather(w2_ref, lambda p: (expand_ref, shrink_ref)[p], sems[6:], to)
    own_copy = lambda p: pltpu.make_async_copy(gather2.piece(p), w2_ref.at[p, gather2.z, gather2.x, gather2.core], local_sem.at[p])

    @at_step(0)
    def _():
        greet(to)
        for i in range(count):
            x_copy(i).start()
        for p in range(4):
            gather1.along_z(p)
            w[p, gather1.z, gather1.x, gather1.core] = gather1.piece(p)[...]
        dk_sum[...] = jnp.zeros_like(dk_sum)
        dv_sum[...] = jnp.zeros_like(dv_sum)
        put_tables(*tables)
        for p in range(4):
            gather1.across_x(p)
        for p in range(4):
            gather1.across_core(p)
        for p in range(2):
            own_copy(p).start()
            gather2.along_z(p)
        for p in range(4):
            gather1.end(p)

    def pass_on(p):
        own_copy(p).wait()
        gather2.across_x(p)

    for first, second, what, p in ((5, 1, pass_on, 0), (8, 3, pass_on, 1), (9, 5, gather2.across_core, 0), (13, 8, gather2.across_core, 1)):
        pl.when(step == n + jnp.where(t == 0, first, second))(functools.partial(what, p))

    @at_step(n + 2 * blocks * pairs - 1)
    def _():
        for p in range(2):
            gather2.end(p)

    for i in range(count):

        @at_step(count + i)
        def _():
            x_copy(i).wait()
            if i >= count - blocks:
                g_copy(i - count + blocks).start()

    @pl.when(step < n)
    def _():
        choose(step < count, x_other, x_ref, lambda: x_got[step - count])
        n1 = norms(x_other[...], [v0_ref, v1_ref, v2_ref, v3_ref], n1_ref, n2_ref, st_ref)
        at = pl.ds(pl.multiple_of(lax.rem(step * ROWS + t * own, 2 * own), ROWS), ROWS)
        here = [r[at, :] for r in tables]
        for part, ref in enumerate((q_all, k_all, v_all)):
            y = project(part, n1, weight(part), b_ref, here)
            for p in range(pairs):
                ref[p, at, :] = y[:, p * 128 : (p + 1) * 128]

    later = step - n
    turn_of, pair = lax.div(later, pairs), lax.rem(later, pairs)
    block = lax.rem(turn_of + t * blocks, 2 * blocks)

    @pl.when(jnp.logical_and(later >= 0, pair == 0))
    def _():
        for i in range(blocks):

            @pl.when(turn_of == blocks + i)
            def _():
                g_copy(i).wait()

        choose(turn_of < blocks, g_other, g_ref, lambda: g_got[turn_of - blocks])
        y = dot(g_other[...], weight(3)).astype(bf16)
        for p in range(pairs):
            do_all[p] = y[:, p * 128 : (p + 1) * 128]

    for i in range(2 * blocks):

        @pl.when(jnp.logical_and(later >= 0, block == i))
        def _():
            q = q_all[pair, i * BLOCK : (i + 1) * BLOCK, :]
            o_ref[...], dq_ref[...] = attend(i, q, do_all[pair], k_all.at[pair], v_all.at[pair], dk_sum.at[pair], dv_sum.at[pair], tables, BLOCK)

    @pl.when(turn_of == 2 * blocks - 1)
    def _():
        put_sums(dk_ref, dv_ref, dk_sum.at[pair], dv_sum.at[pair], tables, BLOCK)

    @at_step(n)
    def _():
        for p in range(4):
            w_ref[:, lanes(p)] = weight(p)


def head_call(x, grads, project, dense, expand, shrink, vec, bias):
    own, d = x.shape
    (part, width), hidden = dense.shape, shrink.shape[1]
    pairs, g = width // 128, 2 * own
    n, blocks = g // ROWS, own // BLOCK
    count = n // 2
    last = lambda i, top: jnp.clip(i, 0, top - 1)
    rows = lambda c: pl.BlockSpec((ROWS, c), lambda i: (last(i, n), 0))
    other_rows = pl.BlockSpec((ROWS, d), lambda i: (last(i - count, count), 0))
    own_rows = pl.BlockSpec((ROWS, d), lambda i: (last(i, count), 0))
    at = lambda i: last(lax.div(jnp.maximum(i - n, 0), pairs), 2 * blocks)
    pair = lambda i: lax.rem(jnp.maximum(i - n, 0), pairs)
    out = pl.BlockSpec((BLOCK, 128), lambda i: (at(i), pair(i)))
    sums = pl.BlockSpec((LEN, 128), lambda i: (0, jnp.where(at(i) == 2 * blocks - 1, pair(i), 0)))
    any_spec = pl.BlockSpec(memory_space=pl.ANY)
    head_rows = lambda: pltpu.VMEM((pairs, LEN, 128), bf16)
    head_sums = lambda: pltpu.VMEM((pairs, 128, LEN), f32)
    return call(
        functools.partial(head_kernel, own=own, pairs=pairs),
        (n + 2 * blocks * pairs,),
        [own_rows, any_spec, pl.BlockSpec((BLOCK, d), lambda i: (last(at(i), blocks), 0)), any_spec]
        + [pl.BlockSpec(project.shape, lambda i: (0, 0, 0), pipeline_mode=pl.Buffered(1))]
        + [held(*a.shape) for a in (dense, expand, shrink, *vec, bias)],
        [rows(d), rows(d), rows(2), out, out, sums, sums, held(d, 4 * width), other_rows]
        + [pl.BlockSpec((BLOCK, d), lambda i: (last(at(i) - blocks, blocks), 0)), any_spec],
        [shape(g, d, bf16), shape(g, d, bf16), shape(g, 2, f32)]
        + [shape(g, width, bf16)] * 4
        + [shape(d, 4 * width, bf16), shape(own, d, bf16), shape(own, d, bf16), jax.ShapeDtypeStruct((2, 4, 2, 2, part, hidden), bf16)],
        [
            pltpu.VMEM((4, 4, 2, 2, part, width), bf16),
            pltpu.VMEM((count, ROWS, d), bf16),
            pltpu.VMEM((blocks, BLOCK, d), bf16),
            head_rows(),
            head_rows(),
            head_rows(),
            pltpu.VMEM((pairs, BLOCK, 128), bf16),
            head_sums(),
            head_sums(),
        ]
        + [pltpu.VMEM((LEN, 128), f32)] * 3
        + [pltpu.SemaphoreType.DMA((2,))]
        + sem_pair(count)
        + sem_pair(blocks)
        + Gather.scratch(4)
        + Gather.scratch(2),
        6 * g * d * width + 24 * g * LEN * width,
        0,
        collective=2,
    )(x, x, grads, grads, project, dense, expand, shrink, *vec, bias)


def normal_of(refs, st_ref, count):
    return (pick(refs, count).astype(f32) - st_ref[:, 0:1]) * st_ref[:, 1:2]


def project_back_kernel(shift, dq_ref, dk_ref, dv_ref, ctx_ref, n1_ref, x_ref, y_ref, st_ref, go_ref, gt_ref, gain_ref, w_ref, s_ref, send_ref, keep_ref, cols_ref, bias_ref, acc, *, count, fsdp):
    @at_first()
    def _():
        acc[...] = jnp.zeros_like(acc)
        cols_ref[...] = jnp.zeros_like(cols_ref)
        bias_ref[...] = jnp.zeros_like(bias_ref)

    n1 = n1_ref[...]
    width = dk_ref.shape[1]
    s = 0.0
    for part, joined in enumerate((dq_ref[...], dk_ref[...], dv_ref[...])):
        lanes = slice(part * width, (part + 1) * width)
        bias_ref[part : part + 1, :] += jnp.sum(joined.astype(f32), axis=0, keepdims=True)
        s = s + dot(joined, w_ref[:, lanes], 1, 1)
        acc[:, lanes] += dot(n1, joined, 0, 0)
    acc[:, 3 * width :] += dot(pick((go_ref, gt_ref), count), ctx_ref[...], 0, 0)
    normal = normal_of((x_ref, y_ref), st_ref, count)
    cols_ref[0:1, :] += jnp.sum(s * normal, axis=0, keepdims=True)
    cols_ref[1:2, :] += jnp.sum(s, axis=0, keepdims=True)
    s_ref[...] = s * gain_ref[...]

    @at_last()
    def _():
        put_blocks(fsdp, (send_ref, keep_ref), acc)


def project_back_call(shift, fsdp, dq, dk, dv, ctx, n1, x, st, grads, vec, w1, rows=256):
    g, d = n1.shape
    width = dk.shape[1]
    n, count = g // rows, x[0].shape[0] // rows
    return call(
        functools.partial(project_back_kernel, count=count, fsdp=fsdp),
        (n,),
        [own_order(rows, width), *[seq_order(rows, width, n)] * 2, own_order(rows, width), own_order(rows, d)]
        + both(rows, d, count)
        + [own_order(rows, 2)]
        + both(rows, d, count)
        + [held(1, d), held(d, 3 * width)],
        [own_order(rows, d), *[pieces(d, 4 * width)[0]] * 2, held(2, d), held(3, width)],
        [shape(g, d, f32), *[pieces(d, 4 * width)[1]] * 2, shape(2, d, f32), shape(3, width, f32)],
        [pltpu.VMEM((d, 4 * width), f32)],
        14 * g * d * width,
    )(shift, dq, dk, dv, ctx, n1, *x, st, *grads, vec[0], w1)


def feed_forward_kernel(n2_ref, go_ref, gt_ref, ctx_ref, we_ref, ws_ref, wd_ref, be_ref, *refs, count, fsdp, fast):
    if fast:
        x_ref, bias_ref, d_send, d_keep, gp_ref, out_ref, send_ref, keep_ref, dw1_ref, acc, to_owner, from_other, *scratch = refs
        to = neighbours()
        reduce = Reduce(d_send, kept(d_keep, acc.shape[0]), dw1_ref, scratch[2:], to)
        row_copy = lambda b: remote(to_owner.at[b], from_other.at[b], scratch[:2], b, to["y"])
    else:
        gp_ref, out_ref, others_ref, send_ref, keep_ref, acc = refs
    step = pl.program_id(0)

    @at_first()
    def _():
        acc[...] = jnp.zeros_like(acc)
        if fast:
            greet(to)
            for p in range(PIECES):
                reduce.across_core(p)

    if fast:
        for at, what in ((1, "x"), (3, 0), (5, 1), (7, "end")):

            @at_step(at)
            def _():
                for p in range(PIECES) if what in ("x", "end") else [what]:
                    {"x": reduce.across_x, "end": reduce.end}.get(what, reduce.along_z)(p)

        for b in range(count):

            @at_step(b + 1)
            def _():
                row_copy(b).start()

    own = step >= count
    n2, g = n2_ref[...], jnp.where(own, go_ref[...], gt_ref[...])
    branch = dot(ctx_ref[...], wd_ref[...], 1, 1)
    act, slope = gelu_parts(dot(n2, we_ref[...]) + be_ref[...])
    act = act.astype(bf16)
    gp_ref[...] = slope.astype(bf16)
    branch = branch + dot(act, ws_ref[...], 1, 1)
    acc[...] += dot(g, act, 0, 0)
    if fast:

        @pl.when(jnp.logical_not(own))
        def _():
            to_owner[step] = branch.astype(bf16)

        for b in range(count):

            @at_step(b + count)
            def _():
                row_copy(b).wait()
                out_ref[...] = (x_ref[...].astype(f32) + (branch + from_other[b].astype(f32)) + bias_ref[...]).astype(bf16)

    else:
        put((others_ref, out_ref), count, branch.astype(bf16))

    @at_last()
    def _():
        put_blocks(fsdp, (send_ref, keep_ref), acc)


def feed_forward_call(fsdp, n2, grads, ctx, w2, w1, be, more=None, rows=256):
    g, d = n2.shape
    hidden, width = w2.shape[2], ctx.shape[1]
    own = grads[0].shape[0]
    n = g // rows
    count = own // rows if more else (g - own) // rows
    first = lambda c: pl.BlockSpec((rows, c), lambda i, *s: (jnp.minimum(i, count - 1), 0))
    second = lambda c: pl.BlockSpec((rows, c), lambda i, *s: (jnp.maximum(i - count, 0), 0))
    turned = lambda c: pl.BlockSpec((rows, c), lambda i, *s: ((i + own // rows) % n, 0))
    ins = [turned(d), second(d), first(d), turned(width), weight_of(w2, 0), weight_of(w2, 1), held(d, width, 3), held(1, hidden)]
    half = pieces(d, hidden)
    acc = pltpu.VMEM((d, hidden), f32)
    flops = g * d * (6 * hidden + 2 * width)
    kernel = functools.partial(feed_forward_kernel, count=count, fsdp=fsdp, fast=bool(more))
    args = (n2, *grads, ctx, w2, w2, w1, be)
    if not more:
        outs = [turned(hidden), second(d), first(d), half[0], half[0]]
        shapes = [shape(g, hidden, bf16), shape(own, d, bf16), shape(g - own, d, bf16), half[1], half[1]]
        return call(kernel, (n,), ins, outs, shapes, [acc], flops, 0)(*args)
    part = d // 16
    ins += [second(d), held(1, d), pl.BlockSpec(memory_space=pl.ANY), pieces(d, 4 * width)[0]]
    parts = (4, part, width)
    outs = [turned(hidden), second(d), half[0], half[0], pl.BlockSpec(parts, lambda i: (0, 0, 0), pipeline_mode=pl.Buffered(1))]
    shapes = [shape(g, hidden, bf16), shape(own, d, bf16), half[1], half[1], jax.ShapeDtypeStruct(parts, f32)]
    rows_buffer = pltpu.VMEM((count, rows, d), bf16)
    scratch = [acc, rows_buffer, rows_buffer] + sem_pair(count) + Reduce.scratch(d, 4 * width)
    return call(kernel, (n,), ins, outs, shapes, scratch, flops, 0, collective=0)(*args, *more)


def feed_back_kernel(n2_ref, go_ref, gt_ref, gp_ref, s1_ref, x_ref, y_ref, st_ref, gain_ref, we_ref, ws_ref, *refs, count, last, fsdp):
    s_refs = refs[: 1 + last]
    send_ref, keep_ref, cols_ref, bias_ref, acc = refs[1 + last :]

    @at_first()
    def _():
        acc[...] = jnp.zeros_like(acc)
        cols_ref[...] = jnp.zeros_like(cols_ref)
        bias_ref[...] = jnp.zeros_like(bias_ref)

    n2, g = n2_ref[...], pick((go_ref, gt_ref), count)
    pre_grad = (dot(g, ws_ref[...]) * gp_ref[...].astype(f32)).astype(bf16)
    bias_ref[...] += jnp.sum(pre_grad.astype(f32), axis=0, keepdims=True)
    s = dot(pre_grad, we_ref[...], 1, 1)
    acc[...] += dot(n2, pre_grad, 0, 0)
    normal = normal_of((x_ref, y_ref), st_ref, count)
    cols_ref[0:1, :] += jnp.sum(s * normal, axis=0, keepdims=True)
    cols_ref[1:2, :] += jnp.sum(s, axis=0, keepdims=True)
    s = s1_ref[...] + s * gain_ref[...]
    if last:
        put(s_refs, count, s.astype(bf16))
    else:
        s_refs[0][...] = s

    @at_last()
    def _():
        put_blocks(fsdp, (send_ref, keep_ref), acc)


def feed_back_call(fsdp, n2, grads, gp, s1, x, st, vec, w2, half, last, rows=256):
    g, d = n2.shape
    hidden = gp.shape[1] // 2
    own = x[0].shape[0]
    n, count = g // rows, own // rows
    return call(
        functools.partial(feed_back_kernel, count=count, last=last, fsdp=fsdp),
        (n,),
        [own_order(rows, d)]
        + both(rows, d, count)
        + [pl.BlockSpec((rows, hidden), lambda i, *s: (i, half)), own_order(rows, d)]
        + both(rows, d, count)
        + [own_order(rows, 2), held(1, d), weight_of(w2, 0, half), weight_of(w2, 1, half)],
        (both(rows, d, count) if last else [own_order(rows, d)]) + [pieces(d, hidden)[0]] * 2 + [held(2, d), held(1, hidden)],
        ([shape(own, d, bf16), shape(g - own, d, bf16)] if last else [shape(g, d, f32)])
        + [pieces(d, hidden)[1]] * 2
        + [shape(2, d, f32), shape(1, hidden, f32)],
        [pltpu.VMEM((d, hidden), f32)],
        6 * g * d * hidden,
        0,
    )(n2, *grads, gp, s1, *x, st, vec[2], w2, w2)


TAIL = 7
LAST_PIECES = 4


def feed_back_last_kernel(
    n2_ref, go_ref, gt_ref, gp_ref, s1_ref, x_ref, y_ref, st_ref, gain_ref, we_ref, ws_ref, d_send, d_keep, cols_ref, bias_ref,
    grad_ref, dws_ref, dwe_ref, sum_ref,
    acc, to_owner, from_other, own_s, e_send, parts, parts_got, *scratch, count,
):
    n = 2 * count
    d = acc.shape[0]
    step = pl.program_id(0)
    to = neighbours()
    row_sems, sum_sems, scratch = scratch[0:2], scratch[2:4], scratch[4:]
    size = len(scratch) // 2
    shrink = Reduce(d_send, kept(d_keep, d), dws_ref, scratch[:size], to)

    def from_acc(p, j):
        rows = d // 16
        return acc[pl.ds(pl.multiple_of(block_order(j) * rows, rows), rows), expand.cols(p)]

    expand = Reduce(e_send, lambda p, j: from_acc(p, 8 + j), dwe_ref, scratch[size:], to)
    small = SumAll(parts, parts_got, sum_sems, to)
    row_copy = lambda b: remote(to_owner.at[b], from_other.at[b], row_sems, b, to["y"])
    normal = (jnp.where(step < count, y_ref[...], x_ref[...]).astype(f32) - st_ref[:, 0:1]) * st_ref[:, 1:2]

    @at_step(0)
    def _():
        acc[...] = jnp.zeros_like(acc)
        parts[0] = jnp.zeros_like(sum_ref)
        parts[0, 0:2, :] = cols_ref[...]
        wide = bias_ref.shape[1]
        for r in range(3):
            at = r * wide % d
            parts[0, 5 + r * wide // d : 6 + r * wide // d, at : at + wide] = bias_ref[r : r + 1, :]
        greet(to)
        for p in range(PIECES):
            shrink.across_core(p)

    @at_step(1)
    def _():
        for p in range(PIECES):
            shrink.across_x(p)

    for p, at in enumerate((4, 6)):
        pl.when(step == at)(functools.partial(shrink.along_z, p))
    for b in range(count):

        @at_step(b + 1)
        def _():
            row_copy(b).start()

    @pl.when(step < n)
    def _():
        own = step >= count
        n2, g = n2_ref[...], jnp.where(own, go_ref[...], gt_ref[...])
        pre_grad = (dot(g, ws_ref[...]) * gp_ref[...].astype(f32)).astype(bf16)
        bias = jnp.sum(pre_grad.astype(f32), axis=0, keepdims=True)
        for r in range(pre_grad.shape[1] // d):
            parts[0, 7 + r : 8 + r, :] += bias[:, r * d : (r + 1) * d]
        s = dot(pre_grad, we_ref[...], 1, 1)
        acc[...] += dot(n2, pre_grad, 0, 0)
        parts[0, 2:3, :] += jnp.sum(s * normal, axis=0, keepdims=True)
        parts[0, 3:4, :] += jnp.sum(s, axis=0, keepdims=True)
        s = s1_ref[...] + s * gain_ref[...]

        @pl.when(own)
        def _():
            own_s[step - count] = s
            parts[0, 4:5, :] += jnp.sum(g.astype(f32), axis=0, keepdims=True)

        @pl.when(jnp.logical_not(own))
        def _():
            to_owner[step] = s.astype(bf16)

    @at_step(n)
    def _():
        small.start(0)
        for p in range(LAST_PIECES):
            for j in range(8):
                e_send[p, expand.block(j)] = from_acc(p, j).astype(bf16)
        for p in range(LAST_PIECES):
            expand.across_core(p)

    @at_step(n + 1)
    def _():
        small.turn(0)
        for p in range(LAST_PIECES):
            expand.across_x(p)

    for p in range(LAST_PIECES):

        @at_step(n + 2 + p)
        def _():
            if p < 3:
                small.turn(p + 1)
            else:
                sum_ref[...] = small.end(5)
            expand.along_z(p)

    @at_step(n + 2)
    def _():
        for p in range(PIECES):
            shrink.end(p)

    for b in range(count):

        @at_step(n + b)
        def _():
            row_copy(b).wait()
            s = own_s[b] + from_other[b].astype(f32)
            centred = s - jnp.mean(s, axis=1, keepdims=True) - normal * jnp.mean(s * normal, axis=1, keepdims=True)
            grad_ref[...] = go_ref[...].astype(f32) + st_ref[:, 1:2] * centred

    @at_step(n + TAIL - 1)
    def _():
        for p in range(LAST_PIECES):
            expand.end(p)


def feed_back_last_call(n2, grads, gp, s1, x, st, vec, w2, dws, cols, bias, rows=256):
    g, d = n2.shape
    hidden = gp.shape[1]
    own = x[0].shape[0]
    n, count = g // rows, own // rows
    part = d // 16
    first = lambda c: pl.BlockSpec((rows, c), lambda i: (jnp.minimum(i, count - 1), 0))
    second = lambda c: pl.BlockSpec((rows, c), lambda i: (jnp.where(i < n, jnp.maximum(i - count, 0), jnp.minimum(i - n, count - 1)), 0))
    turned = lambda c: pl.BlockSpec((rows, c), lambda i: (jnp.where(i < n, lax.rem(i + count, n), jnp.minimum(i - n, count - 1)), 0))
    turned_once = lambda c: pl.BlockSpec((rows, c), lambda i: (lax.rem(jnp.minimum(i, n - 1) + count, n), 0))
    ins = [turned_once(d), second(d), first(d), turned_once(hidden), turned_once(d), second(d), first(d), turned(2), held(1, d)]
    ins += [weight_of(w2, 0), weight_of(w2, 1), pl.BlockSpec(memory_space=pl.ANY), pieces(d, hidden)[0], held(2, d), held(*bias.shape)]
    small = jax.ShapeDtypeStruct((16, d), f32)
    outs = [pl.BlockSpec((rows, d), lambda i: (jnp.clip(i - n, 0, count - 1), 0)), held(part, hidden), held(part, hidden), held(*small.shape)]
    shapes = [shape(own, d, f32), shape(part, hidden, f32), shape(part, hidden, f32), shape(*small.shape, f32)]
    rows_buffer = lambda dtype: pltpu.VMEM((count, rows, d), dtype)
    sums = pltpu.VMEM((5, *small.shape), f32)
    scratch = [pltpu.VMEM((d, hidden), f32), rows_buffer(bf16), rows_buffer(bf16), rows_buffer(f32)]
    scratch += [pltpu.VMEM((LAST_PIECES, d // 2, hidden // LAST_PIECES), bf16), sums, sums]
    scratch += sem_pair(count) + sem_pair(5) + Reduce.scratch(d, hidden) + Reduce.scratch(d, hidden, LAST_PIECES)
    return call(functools.partial(feed_back_last_kernel, count=count), (n + TAIL,), ins, outs, shapes, scratch, 6 * g * d * hidden, 0, collective=1)(
        n2, *grads, gp, s1, *x, st, vec[2], w2, w2, *dws, cols, bias
    )


def rotary_tables():
    half = ROT // 2
    position = jnp.arange(LEN).astype(f32)
    inverse = 10000.0 ** (-(jnp.arange(half).astype(f32) * 2.0) / ROT)
    angle = position[:, None] * inverse[None, :]
    cos, sin = jnp.cos(angle), jnp.sin(angle)
    rest = jnp.zeros((LEN, HS - ROT), f32)
    none = jnp.zeros((LEN, half), f32)
    period = lambda *a: jnp.tile(jnp.concatenate(a, axis=1), (1, 128 // HS))
    return period(cos, cos, rest + 1.0), period(-sin, none, rest), period(none, sin, rest)


def join(a):
    return jnp.concatenate(list(a), axis=1)


def make_body(fsdp, tp):
    fast = (fsdp, tp) == (16, 2)

    def body(inputs, cotangent, first_gain, first_shift, second_gain, second_shift, project_weight, project_bias, dense_weight, dense_bias, expand_weight, expand_bias, shrink_weight, shrink_bias):
        rows, d = inputs.shape
        width = dense_weight.shape[0]
        hidden = shrink_weight.shape[0]
        part = project_weight.shape[0]
        me = lax.axis_index("tp")
        split = lambda a: (a[:rows], a[rows:])
        zero = jnp.zeros((1,), jnp.int32)
        vec = [a[None] for a in (first_gain, first_shift, second_gain, second_shift)]
        if fast:
            shift = (me * rows).astype(jnp.int32)[None]
            n1, n2, st, ctx, dq, dk, dv, w1, x, grads, w2 = head_call(
                inputs, cotangent, project_weight.transpose(1, 0, 2), dense_weight.T, expand_weight, shrink_weight.T, vec, project_bias
            )
            w2 = w2.reshape(2, d, hidden)
            x, grads = (inputs, x), (cotangent, grads)
        else:
            shift = zero
            gather = lambda a: lax.all_gather(a, "fsdp", axis=0, tiled=True)
            w1 = gather(jnp.concatenate([project_weight.reshape(part, 3 * width), dense_weight.T], axis=1))
            w2 = jnp.stack([gather(expand_weight), gather(shrink_weight.T)])
            tables = rotary_tables()
            x = split(lax.all_gather(inputs, "tp", axis=0, tiled=True))
            grads = split(lax.all_gather(cotangent, "tp", axis=0, tiled=True))
            n1, n2, st, q, k, v = qkv_call(shift, x, vec, w1, project_bias, tables, width)
            do = context_grad_call(zero, jnp.concatenate(grads), w1, width)
            ctx, dq, dk, dv = attention_call(q, k, v, do, tables)
        s, *dw1, cols1, bias1 = project_back_call(shift, fsdp, dq, dk, dv, ctx, n1, x, st, grads, vec, w1)
        out_bias = dense_bias + shrink_bias
        if fast:
            gp, output, *dws, dw1 = feed_forward_call(fsdp, n2, grads, ctx, w2, w1, expand_bias[None], (inputs, out_bias[None], *dw1))
        else:
            gp, *branch = feed_forward_call(fsdp, n2, grads, ctx, w2, w1, expand_bias[None])
            branch, dws = branch[:2], branch[2:]
        if fast:
            input_grad, dws, dwe, small = feed_back_last_call(n2, grads, gp, s, x, st, vec, w2, dws, cols1, bias1)
            cols, local = small[:5], jnp.concatenate([small[5:7].reshape(-1)[: 3 * width], small[7:9].reshape(-1)])
        else:
            s, *dwe, cols2, bias2 = feed_back_call(fsdp, n2, grads, gp, s, x, st, vec, w2, 0, False)
            *s, send, keep, cols3, bias3 = feed_back_call(fsdp, n2, grads, gp, s, x, st, vec, w2, 1, True)
            over = lambda a, axis: lax.psum_scatter(jnp.concatenate(a), axis, scatter_dimension=0, tiled=True).astype(f32)
            scatter = lambda pair: over([join(a) for a in pair], "fsdp")
            s = over(s, "tp")
            own_rows = inputs.astype(f32)
            output = (own_rows + over(branch, "tp") + out_bias).astype(bf16)
            own_st = lax.dynamic_slice_in_dim(st, me * rows, rows, 0)
            own_bias = jnp.sum(cotangent.astype(f32), axis=0, keepdims=True)
            cols = lax.psum(jnp.concatenate([cols1, cols2 + cols3, own_bias]), ("fsdp", "tp"))
            local = lax.psum(jnp.concatenate([bias1.reshape(-1), bias2.reshape(-1), bias3.reshape(-1)]), "fsdp")
            dw1 = scatter(dw1).reshape(part, 4, width).transpose(1, 0, 2)
            dws, dwe = scatter(dws), jnp.concatenate([scatter(dwe), scatter((send, keep))], axis=1)
            normal = (own_rows - own_st[:, 0:1]) * own_st[:, 1:2]
            term = own_st[:, 1:2] * (s - jnp.mean(s, axis=1, keepdims=True) - normal * jnp.mean(s * normal, axis=1, keepdims=True))
            input_grad = cotangent.astype(f32) + term
        return (
            output,
            input_grad,
            cols[0],
            cols[1],
            cols[2],
            cols[3],
            dw1[:3].transpose(1, 0, 2),
            local[: 3 * width].reshape(3, width),
            dw1[3].T,
            cols[4],
            dwe,
            local[3 * width :],
            dws.T,
            cols[4],
        )

    return body


def solution(mesh):
    rows, rep = P(("fsdp", "tp"), None), P()
    return jax.shard_map(
        make_body(mesh.shape["fsdp"], mesh.shape["tp"]),
        mesh=mesh,
        in_specs=(rows, rows, rep, rep, rep, rep, P("fsdp", None, "tp"), P(None, "tp"), P("tp", "fsdp"), rep, P("fsdp", "tp"), P("tp"), P("tp", "fsdp"), rep),
        out_specs=(rows, rows, rep, rep, rep, rep, P("fsdp", None, "tp"), P(None, "tp"), P("tp", "fsdp"), rep, P("fsdp", "tp"), P("tp"), P("tp", "fsdp"), rep),
        check_vma=False,
    )
```

```python
import functools

import jax
import jax.numpy as jnp
from jax import lax
from jax.experimental import pallas as pl
from jax.experimental.pallas import tpu as pltpu
from jax.sharding import PartitionSpec as P

f32, bf16 = jnp.float32, jnp.bfloat16
HS = 64
ROT = 16
LEN = 2048
EPS = 1e-05
NEG = -1e30
VMEM_LIMIT = 60 << 20
PIECES = 2
ERFC = (
    0.22567586308569043,
    0.22566953354787173,
    0.20784372127485384,
    0.1685348386069925,
    0.14145750936579315,
    -0.005660950942278366,
    0.16914715407444447,
    -0.18293900460081808,
    0.050271460956987875,
)


def dot(a, b, ca=1, cb=0):
    return lax.dot_general(a, b, (((ca,), (cb,)), ((), ())), preferred_element_type=f32)


def gelu_parts(x):
    t = pl.reciprocal(1.0 + (0.4 * 0.5**0.5) * jnp.abs(x))
    poly = jnp.full_like(t, ERFC[-1])
    for c in ERFC[-2::-1]:
        poly = poly * t + c
    e = jnp.exp(-0.5 * (x * x))
    tail = (0.5 * t) * poly * e
    cdf = jnp.where(x < 0, tail, 1.0 - tail)
    return x * cdf, cdf + x * (e * 0.3989422804014327)


def call(kernel, grid, in_specs, out_specs, out_shape, scratch, flops, scalars=1, collective=None):
    size = lambda a: a.dtype.itemsize * a.size
    return lambda *args: pl.pallas_call(
        kernel,
        grid_spec=pltpu.PrefetchScalarGridSpec(num_scalar_prefetch=scalars, grid=grid, in_specs=in_specs, out_specs=out_specs, scratch_shapes=scratch),
        out_shape=out_shape,
        compiler_params=pltpu.CompilerParams(vmem_limit_bytes=VMEM_LIMIT, collective_id=collective, has_side_effects=collective is not None),
        cost_estimate=pl.CostEstimate(flops=int(flops), transcendentals=0, bytes_accessed=sum(map(size, args)) + sum(map(size, out_shape))),
    )(*args)


def held(rows, cols, col_block=0):
    return pl.BlockSpec((rows, cols), lambda *i: (0, col_block), pipeline_mode=pl.Buffered(1))


def weight_of(w2, p, half=None):
    _, rows, cols = w2.shape
    if half is not None:
        cols = cols // 2
    return pl.BlockSpec((None, rows, cols), lambda *i: (p, 0, half or 0), pipeline_mode=pl.Buffered(1))


def shape(rows, cols, dtype):
    return jax.ShapeDtypeStruct((rows, cols), dtype)


def both(rows, cols, count):
    return [
        pl.BlockSpec((rows, cols), lambda i, *s: (jnp.minimum(i, count - 1), 0)),
        pl.BlockSpec((rows, cols), lambda i, *s: (jnp.maximum(i - count, 0), 0)),
    ]


def own_order(rows, cols):
    return pl.BlockSpec((rows, cols), lambda i, *s: (i, 0))


def seq_order(rows, cols, n):
    return pl.BlockSpec((rows, cols), lambda i, shift, *s: ((i + shift[0] // rows) % n, 0))


def pick(refs, count):
    return jnp.where(pl.program_id(0) < count, refs[0][...], refs[1][...])


def put(refs, count, value):
    for ref, here in zip(refs, (pl.program_id(0) < count, pl.program_id(0) >= count)):

        @pl.when(here)
        def _():
            ref[...] = value


def at_first():
    return pl.when(pl.program_id(0) == 0)


def at_last():
    return pl.when(pl.program_id(0) == pl.num_programs(0) - 1)


def block_order(j):
    f = lax.axis_index("fsdp")
    z, x, core = lax.div(f, 4), lax.rem(lax.div(f, 2), 2), lax.rem(f, 2)
    other_core, other_x, k = 1 - j // 8, 1 - j // 4 % 2, j % 4
    x = 1 - x if other_x else x
    core = 1 - core if other_core else core
    return lax.rem(z + k, 4) * 4 + x * 2 + core


def put_blocks(fsdp, refs, acc):
    size, wide = acc.shape[0] // fsdp, acc.shape[1] // PIECES
    for j in range(fsdp):
        rows = pl.ds(pl.multiple_of(block_order(j) * size, size), size) if fsdp == 16 else slice(j * size, (j + 1) * size)
        at = j % (fsdp // 2) * size
        for p in range(PIECES):
            refs[j // (fsdp // 2)][p, at : at + size, :] = acc[rows, p * wide : (p + 1) * wide].astype(bf16)


def pieces(d, cols):
    dims = (PIECES, d // 2, cols // PIECES)
    return pl.BlockSpec(dims, lambda *i: (0, 0, 0), pipeline_mode=pl.Buffered(1)), jax.ShapeDtypeStruct(dims, bf16)


def neighbours():
    f, t = lax.axis_index("fsdp"), lax.axis_index("tp")
    core, x = lax.rem(f, 2), lax.rem(lax.div(f, 2), 2)
    around = [(lax.rem(f + 4 * k, 16), t) for k in range(1, 4)]
    z_pair = (f + 4 - 8 * lax.rem(lax.div(f, 4), 2), t)
    return {"core": (f + 1 - 2 * core, t), "x": (f + 2 - 4 * x, t), "y": (f, 1 - t), "z": around, "z_pair": z_pair}


def greet(to):
    barrier = pltpu.get_barrier_semaphore()
    peers = [to["core"], to["x"], to["y"], *to["z"]]
    for peer in peers:
        pl.semaphore_signal(barrier, inc=1, device_id=peer, device_id_type=pl.DeviceIdType.MESH)
    pl.semaphore_wait(barrier, len(peers))


def remote(src, dst, sems, at, peer):
    return pltpu.make_async_remote_copy(
        src_ref=src, dst_ref=dst, send_sem=sems[0].at[at], recv_sem=sems[1].at[at], device_id=peer, device_id_type=pl.DeviceIdType.MESH
    )


def sem_pair(count):
    return [pltpu.SemaphoreType.DMA((count,)), pltpu.SemaphoreType.DMA((count,))]


class Reduce:
    def __init__(self, send, keep, out, scratch, to):
        self.send, self.keep, self.out, self.to = send, keep, out, to
        self.got, self.send2, self.got2, self.send3, self.got3, *sems = scratch
        self.sems = [sems[0:2], sems[2:4], sems[4:6]]
        self.count, rows, self.wide = self.got.shape
        self.rows = rows // 8

    @staticmethod
    def scratch(d, cols, count=PIECES):
        rows, wide = d // 16, cols // count
        buffer = lambda n: pltpu.VMEM((count, n * rows, wide), bf16)
        return [buffer(8), buffer(4), buffer(4), buffer(3), buffer(3)] + sem_pair(count) + sem_pair(count) + sem_pair(3 * count)

    def block(self, j):
        return slice(j * self.rows, (j + 1) * self.rows)

    def emit(self, p, total, add=False):
        if len(self.out.shape) == 2:
            self.out[:, self.cols(p)] = total + self.out[:, self.cols(p)] if add else total
            return
        width = self.out.shape[2]
        for r in range(self.wide // width):
            at, here = p * (self.wide // width) + r, total[:, r * width : (r + 1) * width]
            self.out[at] = here + self.out[at] if add else here

    def cols(self, p):
        return slice(p * self.wide, (p + 1) * self.wide)

    def copy1(self, p):
        return remote(self.send.at[p], self.got.at[p], self.sems[0], p, self.to["core"])

    def copy2(self, p):
        return remote(self.send2.at[p], self.got2.at[p], self.sems[1], p, self.to["x"])

    def copies3(self, p):
        cut = lambda ref, k: ref.at[p, self.block(k)]
        return [remote(cut(self.send3, k), cut(self.got3, k), self.sems[2], 3 * p + k, self.to["z"][k]) for k in range(3)]

    def across_core(self, p):
        self.copy1(p).start()

    def across_x(self, p):
        self.copy1(p).wait()
        for j in range(4):
            self.send2[p, self.block(j)] = (self.keep(p, j) + self.got[p, self.block(j)].astype(f32)).astype(bf16)
        self.copy2(p).start()

    def along_z(self, p):
        self.copy2(p).wait()
        for k in (1, 2, 3, 0):
            total = self.keep(p, 4 + k) + self.got[p, self.block(4 + k)].astype(f32) + self.got2[p, self.block(k)].astype(f32)
            if k:
                self.send3[p, self.block(k - 1)] = total.astype(bf16)
            else:
                self.emit(p, total)
        for copy in self.copies3(p):
            copy.start()

    def end(self, p):
        for copy in self.copies3(p):
            copy.wait()
        got = [self.got3[p, self.block(k)].astype(f32) for k in range(3)]
        self.emit(p, got[0] + got[1] + got[2], add=True)


def kept(ref, d):
    rows = d // 16
    return lambda p, j: ref[p, j * rows : (j + 1) * rows].astype(f32)


class SumAll:
    def __init__(self, parts, got, sems, to):
        self.parts, self.got, self.sems = parts, got, sems
        self.peers = [to["core"], to["x"], to["z"][1], to["z_pair"], to["y"]]

    def copy(self, i):
        return remote(self.parts.at[i], self.got.at[i], self.sems, i, self.peers[i])

    def start(self, i):
        self.copy(i).start()

    def turn(self, i):
        self.copy(i).wait()
        self.parts[i + 1] = self.parts[i] + self.got[i]
        self.copy(i + 1).start()

    def end(self, rows_over_tp):
        last = len(self.peers) - 1
        self.copy(last).wait()
        row = lax.broadcasted_iota(jnp.int32, self.parts.shape[1:], 0)
        return self.parts[last] + jnp.where(row < rows_over_tp, self.got[last], 0.0)


def at_step(i):
    return pl.when(pl.program_id(0) == i)


def turn(y, cos, sin_up, sin_down):
    width = y.shape[1]
    half = ROT // 2
    return y * cos + pltpu.roll(y, width - half, 1) * sin_up + pltpu.roll(y, half, 1) * sin_down


def norms(x, vec, n1_ref, n2_ref, st_ref):
    x = x.astype(f32)
    mean = jnp.mean(x, axis=1, keepdims=True)
    centred = x - mean
    rstd = lax.rsqrt(jnp.mean(centred * centred, axis=1, keepdims=True) + EPS)
    normal = centred * rstd
    st_ref[:, 0:1] = mean
    st_ref[:, 1:2] = rstd
    n1 = (normal * vec[0][...] + vec[1][...]).astype(bf16)
    n1_ref[...] = n1
    n2_ref[...] = (normal * vec[2][...] + vec[3][...]).astype(bf16)
    return n1


def project(part, n1, w, b_ref, tables):
    y = dot(n1, w) + b_ref[part : part + 1, :]
    if part < 2:
        y = turn(y, *[jnp.concatenate([t] * (y.shape[1] // 128), axis=1) for t in tables])
    if part == 0:
        y = y * HS**-0.5
    return y.astype(bf16)


def qkv_kernel(shift, x_ref, y_ref, v0_ref, v1_ref, v2_ref, v3_ref, w_ref, b_ref, c_ref, sa_ref, sb_ref, n1_ref, n2_ref, st_ref, q_ref, k_ref, v_ref, *, count):
    n1 = norms(pick((x_ref, y_ref), count), [v0_ref, v1_ref, v2_ref, v3_ref], n1_ref, n2_ref, st_ref)
    width = q_ref.shape[1]
    for part, ref in enumerate((q_ref, k_ref, v_ref)):
        ref[...] = project(part, n1, w_ref[:, part * width : (part + 1) * width], b_ref, [c_ref[...], sa_ref[...], sb_ref[...]])


def qkv_call(shift, x, vec, w1, bias, tables, width, rows=256):
    d = x[0].shape[1]
    count = x[0].shape[0] // rows
    n = count + x[1].shape[0] // rows
    g = n * rows
    table = pl.BlockSpec((rows, 128), lambda i, shift: (((i + shift[0] // rows) % n) % (LEN // rows), 0))
    return call(
        functools.partial(qkv_kernel, count=count),
        (n,),
        both(rows, d, count) + [held(1, d)] * 4 + [held(d, 3 * width), held(3, width), table, table, table],
        [own_order(rows, d), own_order(rows, d), own_order(rows, 2)] + [seq_order(rows, width, n)] * 3,
        [shape(g, d, bf16), shape(g, d, bf16), shape(g, 2, f32)] + [shape(g, width, bf16)] * 3,
        [],
        6 * g * d * width,
    )(shift, *x, *vec, w1, bias, *tables)


def context_grad_kernel(shift, g_ref, w_ref, do_ref):
    do_ref[...] = dot(g_ref[...], w_ref[...]).astype(bf16)


def context_grad_call(shift, grads, w1, width, rows=512):
    g, d = grads.shape
    return call(
        context_grad_kernel,
        (g // rows,),
        [own_order(rows, d), held(d, width, 3)],
        [own_order(rows, width)],
        [shape(g, width, bf16)],
        [],
        2 * g * d * width,
    )(shift, grads, w1)[0]


def attend(i, q_all, do_all, k_ref, v_ref, dk_sum, dv_sum, tables, block):
    outs, dqs = [], []
    half = block // 2
    parts = [(slice(j * block, (j + 1) * block), 0) for j in range(i)]
    parts += [(slice(i * block, i * block + half), 0), (slice(i * block + half, (i + 1) * block), half)]

    def widen(a, start, fill):
        return a if start == 0 else jnp.concatenate([jnp.full((a.shape[0], start), fill, a.dtype), a], axis=1)

    def gather(op, fill, arrays):
        return functools.reduce(op, [widen(a, start, fill) for a, (_, start) in zip(arrays, parts)])

    for h in range(q_all.shape[1] // HS):
        lanes = slice(h * HS, (h + 1) * HS)
        q, do = q_all[:, lanes], do_all[:, lanes]
        scores = [dot(k_ref[rows, lanes], q[start:], 1, 1) for rows, start in parts]
        for n in (i, i + 1):
            rows, start = parts[n]
            key_pos = lax.broadcasted_iota(jnp.int32, scores[n].shape, 0) + (rows.start - i * block)
            query_pos = lax.broadcasted_iota(jnp.int32, scores[n].shape, 1) + start
            scores[n] = jnp.where(key_pos <= query_pos, scores[n], NEG)
        top = gather(jnp.maximum, NEG, [jnp.max(s, axis=0, keepdims=True) for s in scores])
        weights = [jnp.exp(s - top[:, start:]) for s, (_, start) in zip(scores, parts)]
        scale = 1.0 / gather(jnp.add, 0.0, [jnp.sum(w, axis=0, keepdims=True) for w in weights])
        low = [w.astype(bf16) for w in weights]
        mixed = gather(jnp.add, 0.0, [dot(v_ref[rows, lanes], w, 0, 0) for w, (rows, _) in zip(low, parts)]) * scale
        do_t = do.astype(f32).T * scale
        delta = jnp.sum(mixed * do_t, axis=0, keepdims=True)
        do_t = do_t.astype(bf16)
        q_t = q.astype(f32).T.astype(bf16)
        terms = []
        for n, (rows, start) in enumerate(parts):
            prob_grad = dot(v_ref[rows, lanes], do_t[:, start:])
            score_grad = (weights[n] * (prob_grad - delta[:, start:])).astype(bf16)
            dv_sum[lanes, rows] += dot(do_t[:, start:], low[n], 1, 1)
            dk_sum[lanes, rows] += dot(q_t[:, start:], score_grad, 1, 1)
            terms.append(dot(k_ref[rows, lanes], score_grad, 0, 0))
        outs.append(mixed.T)
        dqs.append(gather(jnp.add, 0.0, terms).T)
    dq = turn_back(jnp.concatenate(dqs, axis=1) * HS**-0.5, tables, slice(i * block, (i + 1) * block))
    return jnp.concatenate(outs, axis=1).astype(bf16), dq.astype(bf16)


def turn_back(y, tables, rows):
    cos, sin_up, sin_down = (t[rows, :] for t in tables)
    return turn(y, cos, -sin_up, -sin_down)


def put_sums(dk_ref, dv_ref, dk_sum, dv_sum, tables, block):
    for i in range(LEN // block):
        rows = slice(i * block, (i + 1) * block)
        dk_ref[rows, :] = turn_back(dk_sum[:, rows].T, tables, rows).astype(bf16)
        dv_ref[rows, :] = dv_sum[:, rows].T.astype(bf16)


def attention_kernel(q_ref, k_ref, v_ref, do_ref, c_ref, sa_ref, sb_ref, o_ref, dq_ref, dk_ref, dv_ref, dk_sum, dv_sum, *, block):
    step = pl.program_id(2)
    tables = (c_ref, sa_ref, sb_ref)

    @pl.when(step == 0)
    def _():
        dk_sum[...] = jnp.zeros_like(dk_sum)
        dv_sum[...] = jnp.zeros_like(dv_sum)

    for i in range(LEN // block):

        @pl.when(step == i)
        def _():
            o_ref[...], dq_ref[...] = attend(i, q_ref[...], do_ref[...], k_ref, v_ref, dk_sum, dv_sum, tables, block)

    @pl.when(step == pl.num_programs(2) - 1)
    def _():
        put_sums(dk_ref, dv_ref, dk_sum, dv_sum, tables, block)


def attention_call(q, k, v, do, tables, block=512):
    g, width = q.shape
    seqs, pairs, count = g // LEN, width // 128, LEN // block
    one = pl.BlockSpec((block, 128), lambda s, h, i: (s * count + i, h))
    whole = pl.BlockSpec((LEN, 128), lambda s, h, i: (s, h))
    return call(
        functools.partial(attention_kernel, block=block),
        (seqs, pairs, count),
        [one, whole, whole, one] + [held(LEN, 128)] * 3,
        [one, one, whole, whole],
        [shape(g, width, bf16)] * 4,
        [pltpu.VMEM((128, LEN), f32), pltpu.VMEM((128, LEN), f32)],
        24 * g * LEN * width,
        0,
    )(q, k, v, do, *tables)


ROWS, BLOCK = 256, 512


INVERSE = [10000.0 ** (-2.0 * j / ROT) for j in range(ROT // 2)]


def put_tables(cos_ref, up_ref, down_ref):
    half = ROT // 2
    lane = lax.rem(lax.broadcasted_iota(jnp.int32, (ROWS, 128), 1), HS)
    inverse = functools.reduce(lambda a, j: jnp.where(lax.rem(lane, half) == j, INVERSE[j], a), range(half), jnp.zeros((ROWS, 128), f32))
    for i in range(LEN // ROWS):
        rows = slice(i * ROWS, (i + 1) * ROWS)
        position = (lax.broadcasted_iota(jnp.int32, (ROWS, 128), 0) + i * ROWS).astype(f32)
        angle = position * inverse
        cos, sin = jnp.cos(angle), jnp.sin(angle)
        cos_ref[rows, :] = jnp.where(lane < ROT, cos, 1.0)
        up_ref[rows, :] = jnp.where(lane < half, -sin, 0.0)
        down_ref[rows, :] = jnp.where(jnp.logical_and(lane >= half, lane < ROT), sin, 0.0)


class Gather:
    def __init__(self, all_ref, piece, sems, to):
        self.all, self.piece, self.to = all_ref, piece, to
        self.sems = [sems[2 * i : 2 * i + 2] for i in range(3)]
        f = lax.axis_index("fsdp")
        self.z, self.x, self.core = lax.div(f, 4), lax.rem(lax.div(f, 2), 2), lax.rem(f, 2)

    @staticmethod
    def scratch(count):
        return sem_pair(3 * count) + sem_pair(count) + sem_pair(count)

    def copies_z(self, p):
        mine = self.all.at[p, self.z, self.x, self.core]
        return [remote(self.piece(p), mine, self.sems[0], 3 * p + k, self.to["z"][k]) for k in range(3)]

    def copy_x(self, p):
        mine = self.all.at[p, :, self.x, self.core]
        return remote(mine, mine, self.sems[1], p, self.to["x"])

    def copy_core(self, p):
        mine = self.all.at[p, :, :, self.core]
        return remote(mine, mine, self.sems[2], p, self.to["core"])

    def along_z(self, p):
        for copy in self.copies_z(p):
            copy.start()

    def across_x(self, p):
        for copy in self.copies_z(p):
            copy.wait()
        self.copy_x(p).start()

    def across_core(self, p):
        self.copy_x(p).wait()
        self.copy_core(p).start()

    def end(self, p):
        self.copy_core(p).wait()


def choose(own, out_ref, own_ref, others):
    @pl.when(own)
    def _():
        out_ref[...] = own_ref[...]

    @pl.when(jnp.logical_not(own))
    def _():
        out_ref[...] = others()


def head_kernel(
    x_ref, x_hbm, g_ref, g_hbm, project_ref, dense_ref, expand_ref, shrink_ref, v0_ref, v1_ref, v2_ref, v3_ref, b_ref,
    n1_ref, n2_ref, st_ref, o_ref, dq_ref, dk_ref, dv_ref, w_ref, x_other, g_other, w2_ref,
    w, x_got, g_got, q_all, k_all, v_all, do_all, dk_sum, dv_sum, c_ref, sa_ref, sb_ref, local_sem, *sems, own, pairs,
):
    step = pl.program_id(0)
    count = own // ROWS
    blocks = own // BLOCK
    n = 2 * count
    t = lax.axis_index("tp")
    to = neighbours()
    tables = (c_ref, sa_ref, sb_ref)
    width = w.shape[-1]
    d = w.shape[1] * w.shape[2] * w.shape[3] * w.shape[4]
    lanes = lambda p: slice(p * width, (p + 1) * width)
    weight = lambda p: w[p].reshape(d, width)
    x_sems, g_sems, sems = sems[0:2], sems[2:4], sems[4:]
    rows_of = lambda ref, i, size: ref.at[pl.ds(i * size, size)]
    x_copy = lambda i: remote(rows_of(x_hbm, i, ROWS), x_got.at[i], x_sems, i, to["y"])
    g_copy = lambda i: remote(rows_of(g_hbm, i, BLOCK), g_got.at[i], g_sems, i, to["y"])
    gather1 = Gather(w, lambda p: dense_ref if p == 3 else project_ref.at[p], sems[:6], to)
    gather2 = Gather(w2_ref, lambda p: (expand_ref, shrink_ref)[p], sems[6:], to)
    own_copy = lambda p: pltpu.make_async_copy(gather2.piece(p), w2_ref.at[p, gather2.z, gather2.x, gather2.core], local_sem.at[p])

    @at_step(0)
    def _():
        greet(to)
        for i in range(count):
            x_copy(i).start()
        for p in range(4):
            gather1.along_z(p)
            w[p, gather1.z, gather1.x, gather1.core] = gather1.piece(p)[...]
        dk_sum[...] = jnp.zeros_like(dk_sum)
        dv_sum[...] = jnp.zeros_like(dv_sum)
        put_tables(*tables)
        for p in range(4):
            gather1.across_x(p)
        for p in range(2):
            own_copy(p).start()
            gather2.along_z(p)
        for p in range(4):
            gather1.across_core(p)
        for p in range(4):
            gather1.end(p)

    def pass_on(p):
        own_copy(p).wait()
        gather2.across_x(p)

    for first, second, what, p in ((5, 1, pass_on, 0), (8, 5, pass_on, 1), (11, 6, gather2.across_core, 0), (14, 12, gather2.across_core, 1)):
        pl.when(step == n + jnp.where(t == 0, first, second))(functools.partial(what, p))

    for i in range(count):

        @at_step(count + i)
        def _():
            x_copy(i).wait()
            if i >= count - blocks:
                g_copy(i - count + blocks).start()

    @pl.when(step < n)
    def _():
        choose(step < count, x_other, x_ref, lambda: x_got[step - count])
        n1 = norms(x_other[...], [v0_ref, v1_ref, v2_ref, v3_ref], n1_ref, n2_ref, st_ref)
        at = pl.ds(pl.multiple_of(lax.rem(step * ROWS + t * own, 2 * own), ROWS), ROWS)
        here = [r[at, :] for r in tables]
        for part, ref in enumerate((q_all, k_all, v_all)):
            y = project(part, n1, weight(part), b_ref, here)
            for p in range(pairs):
                ref[p, at, :] = y[:, p * 128 : (p + 1) * 128]

    later = step - n
    turn_of, pair = lax.div(later, pairs), lax.rem(later, pairs)
    block = lax.rem(turn_of + t * blocks, 2 * blocks)

    @pl.when(jnp.logical_and(later >= 0, pair == 0))
    def _():
        for i in range(blocks):

            @pl.when(turn_of == blocks + i)
            def _():
                g_copy(i).wait()

        choose(turn_of < blocks, g_other, g_ref, lambda: g_got[turn_of - blocks])
        y = dot(g_other[...], weight(3)).astype(bf16)
        for p in range(pairs):
            do_all[p] = y[:, p * 128 : (p + 1) * 128]

    for i in range(2 * blocks):

        @pl.when(jnp.logical_and(later >= 0, block == i))
        def _():
            q = q_all[pair, i * BLOCK : (i + 1) * BLOCK, :]
            o_ref[...], dq_ref[...] = attend(i, q, do_all[pair], k_all.at[pair], v_all.at[pair], dk_sum.at[pair], dv_sum.at[pair], tables, BLOCK)

    @pl.when(turn_of == 2 * blocks - 1)
    def _():
        put_sums(dk_ref, dv_ref, dk_sum.at[pair], dv_sum.at[pair], tables, BLOCK)

    @at_step(n)
    def _():
        for p in range(4):
            w_ref[:, lanes(p)] = weight(p)

    @at_last()
    def _():
        for p in range(2):
            gather2.end(p)


def head_call(x, grads, project, dense, expand, shrink, vec, bias):
    own, d = x.shape
    (part, width), hidden = dense.shape, shrink.shape[1]
    pairs, g = width // 128, 2 * own
    n, blocks = g // ROWS, own // BLOCK
    count = n // 2
    last = lambda i, top: jnp.clip(i, 0, top - 1)
    rows = lambda c: pl.BlockSpec((ROWS, c), lambda i: (last(i, n), 0))
    other_rows = pl.BlockSpec((ROWS, d), lambda i: (last(i - count, count), 0))
    own_rows = pl.BlockSpec((ROWS, d), lambda i: (last(i, count), 0))
    at = lambda i: last(lax.div(jnp.maximum(i - n, 0), pairs), 2 * blocks)
    pair = lambda i: lax.rem(jnp.maximum(i - n, 0), pairs)
    out = pl.BlockSpec((BLOCK, 128), lambda i: (at(i), pair(i)))
    sums = pl.BlockSpec((LEN, 128), lambda i: (0, jnp.where(at(i) == 2 * blocks - 1, pair(i), 0)))
    any_spec = pl.BlockSpec(memory_space=pl.ANY)
    head_rows = lambda: pltpu.VMEM((pairs, LEN, 128), bf16)
    head_sums = lambda: pltpu.VMEM((pairs, 128, LEN), f32)
    return call(
        functools.partial(head_kernel, own=own, pairs=pairs),
        (n + 2 * blocks * pairs,),
        [own_rows, any_spec, pl.BlockSpec((BLOCK, d), lambda i: (last(at(i), blocks), 0)), any_spec]
        + [pl.BlockSpec(project.shape, lambda i: (0, 0, 0), pipeline_mode=pl.Buffered(1))]
        + [held(*a.shape) for a in (dense, expand, shrink, *vec, bias)],
        [rows(d), rows(d), rows(2), out, out, sums, sums, held(d, 4 * width), other_rows]
        + [pl.BlockSpec((BLOCK, d), lambda i: (last(at(i) - blocks, blocks), 0)), any_spec],
        [shape(g, d, bf16), shape(g, d, bf16), shape(g, 2, f32)]
        + [shape(g, width, bf16)] * 4
        + [shape(d, 4 * width, bf16), shape(own, d, bf16), shape(own, d, bf16), jax.ShapeDtypeStruct((2, 4, 2, 2, part, hidden), bf16)],
        [
            pltpu.VMEM((4, 4, 2, 2, part, width), bf16),
            pltpu.VMEM((count, ROWS, d), bf16),
            pltpu.VMEM((blocks, BLOCK, d), bf16),
            head_rows(),
            head_rows(),
            head_rows(),
            pltpu.VMEM((pairs, BLOCK, 128), bf16),
            head_sums(),
            head_sums(),
        ]
        + [pltpu.VMEM((LEN, 128), f32)] * 3
        + [pltpu.SemaphoreType.DMA((2,))]
        + sem_pair(count)
        + sem_pair(blocks)
        + Gather.scratch(4)
        + Gather.scratch(2),
        6 * g * d * width + 24 * g * LEN * width,
        0,
        collective=2,
    )(x, x, grads, grads, project, dense, expand, shrink, *vec, bias)


def normal_of(refs, st_ref, count):
    return (pick(refs, count).astype(f32) - st_ref[:, 0:1]) * st_ref[:, 1:2]


def project_back_kernel(shift, dq_ref, dk_ref, dv_ref, ctx_ref, n1_ref, x_ref, y_ref, st_ref, go_ref, gt_ref, gain_ref, w_ref, s_ref, send_ref, keep_ref, cols_ref, bias_ref, acc, *, count, fsdp):
    @at_first()
    def _():
        acc[...] = jnp.zeros_like(acc)
        cols_ref[...] = jnp.zeros_like(cols_ref)
        bias_ref[...] = jnp.zeros_like(bias_ref)

    n1 = n1_ref[...]
    width = dk_ref.shape[1]
    s = 0.0
    for part, joined in enumerate((dq_ref[...], dk_ref[...], dv_ref[...])):
        lanes = slice(part * width, (part + 1) * width)
        bias_ref[part : part + 1, :] += jnp.sum(joined.astype(f32), axis=0, keepdims=True)
        s = s + dot(joined, w_ref[:, lanes], 1, 1)
        acc[:, lanes] += dot(n1, joined, 0, 0)
    acc[:, 3 * width :] += dot(pick((go_ref, gt_ref), count), ctx_ref[...], 0, 0)
    normal = normal_of((x_ref, y_ref), st_ref, count)
    cols_ref[0:1, :] += jnp.sum(s * normal, axis=0, keepdims=True)
    cols_ref[1:2, :] += jnp.sum(s, axis=0, keepdims=True)
    s_ref[...] = s * gain_ref[...]

    @at_last()
    def _():
        put_blocks(fsdp, (send_ref, keep_ref), acc)


def project_back_call(shift, fsdp, dq, dk, dv, ctx, n1, x, st, grads, vec, w1, rows=256):
    g, d = n1.shape
    width = dk.shape[1]
    n, count = g // rows, x[0].shape[0] // rows
    return call(
        functools.partial(project_back_kernel, count=count, fsdp=fsdp),
        (n,),
        [own_order(rows, width), *[seq_order(rows, width, n)] * 2, own_order(rows, width), own_order(rows, d)]
        + both(rows, d, count)
        + [own_order(rows, 2)]
        + both(rows, d, count)
        + [held(1, d), held(d, 3 * width)],
        [own_order(rows, d), *[pieces(d, 4 * width)[0]] * 2, held(2, d), held(3, width)],
        [shape(g, d, f32), *[pieces(d, 4 * width)[1]] * 2, shape(2, d, f32), shape(3, width, f32)],
        [pltpu.VMEM((d, 4 * width), f32)],
        14 * g * d * width,
    )(shift, dq, dk, dv, ctx, n1, *x, st, *grads, vec[0], w1)


def feed_forward_kernel(n2_ref, go_ref, gt_ref, ctx_ref, we_ref, ws_ref, wd_ref, be_ref, *refs, count, fsdp, fast):
    if fast:
        x_ref, bias_ref, d_send, d_keep, gp_ref, out_ref, late_ref, late_own_ref, send_ref, keep_ref, dw1_ref, acc, to_owner, from_other, *scratch = refs
        to = neighbours()
        reduce = Reduce(d_send, kept(d_keep, acc.shape[0]), dw1_ref, scratch[2:], to)
        row_copy = lambda b: remote(to_owner.at[b], from_other.at[b], scratch[:2], b, to["y"])
    else:
        gp_ref, out_ref, others_ref, send_ref, keep_ref, acc = refs
    step = pl.program_id(0)

    @at_first()
    def _():
        acc[...] = jnp.zeros_like(acc)
        if fast:
            greet(to)
            for p in range(PIECES):
                reduce.across_core(p)

    if fast:
        for at, what in ((1, "x"), (3, 0), (5, 1), (7, "end")):

            @at_step(at)
            def _():
                for p in range(PIECES) if what in ("x", "end") else [what]:
                    {"x": reduce.across_x, "end": reduce.end}.get(what, reduce.along_z)(p)

        for b in range(count - 1):

            @at_step(b + 1)
            def _():
                row_copy(b).start()

    own = step >= count
    n2, g = n2_ref[...], jnp.where(own, go_ref[...], gt_ref[...])
    branch = dot(ctx_ref[...], wd_ref[...], 1, 1)
    act, slope = gelu_parts(dot(n2, we_ref[...]) + be_ref[...])
    act = act.astype(bf16)
    gp_ref[...] = slope.astype(bf16)
    branch = branch + dot(act, ws_ref[...], 1, 1)
    acc[...] += dot(g, act, 0, 0)
    if fast:

        @pl.when(step < count - 1)
        def _():
            to_owner[step] = branch.astype(bf16)

        @at_step(count - 1)
        def _():
            late_ref[...] = branch.astype(bf16)

        @at_last()
        def _():
            late_own_ref[...] = x_ref[...].astype(f32) + (branch + bias_ref[...])

        for b in range(count - 1):

            @at_step(b + count)
            def _():
                row_copy(b).wait()
                out_ref[...] = (x_ref[...].astype(f32) + (branch + from_other[b].astype(f32)) + bias_ref[...]).astype(bf16)

    else:
        put((others_ref, out_ref), count, branch.astype(bf16))

    @at_last()
    def _():
        put_blocks(fsdp, (send_ref, keep_ref), acc)


def feed_forward_call(fsdp, n2, grads, ctx, w2, w1, be, more=None, rows=256):
    g, d = n2.shape
    hidden, width = w2.shape[2], ctx.shape[1]
    own = grads[0].shape[0]
    n = g // rows
    count = own // rows if more else (g - own) // rows
    first = lambda c: pl.BlockSpec((rows, c), lambda i, *s: (jnp.minimum(i, count - 1), 0))
    second = lambda c: pl.BlockSpec((rows, c), lambda i, *s: (jnp.maximum(i - count, 0), 0))
    turned = lambda c: pl.BlockSpec((rows, c), lambda i, *s: ((i + own // rows) % n, 0))
    ins = [turned(d), second(d), first(d), turned(width), weight_of(w2, 0), weight_of(w2, 1), held(d, width, 3), held(1, hidden)]
    half = pieces(d, hidden)
    acc = pltpu.VMEM((d, hidden), f32)
    flops = g * d * (6 * hidden + 2 * width)
    kernel = functools.partial(feed_forward_kernel, count=count, fsdp=fsdp, fast=bool(more))
    args = (n2, *grads, ctx, w2, w2, w1, be)
    if not more:
        outs = [turned(hidden), second(d), first(d), half[0], half[0]]
        shapes = [shape(g, hidden, bf16), shape(own, d, bf16), shape(g - own, d, bf16), half[1], half[1]]
        return call(kernel, (n,), ins, outs, shapes, [acc], flops, 0)(*args)
    part = d // 16
    ins += [second(d), held(1, d), pl.BlockSpec(memory_space=pl.ANY), pieces(d, 4 * width)[0]]
    parts = (4, part, width)
    done = pl.BlockSpec((rows, d), lambda i: (jnp.clip(i - count, 0, count - 2), 0))
    outs = [turned(hidden), done, held(rows, d), held(rows, d), half[0], half[0], pl.BlockSpec(parts, lambda i: (0, 0, 0), pipeline_mode=pl.Buffered(1))]
    shapes = [shape(g, hidden, bf16), shape(own - rows, d, bf16), shape(rows, d, bf16), shape(rows, d, f32)]
    shapes += [half[1], half[1], jax.ShapeDtypeStruct(parts, f32)]
    rows_buffer = pltpu.VMEM((count - 1, rows, d), bf16)
    scratch = [acc, rows_buffer, rows_buffer] + sem_pair(count - 1) + Reduce.scratch(d, 4 * width)
    return call(kernel, (n,), ins, outs, shapes, scratch, flops, 0, collective=0)(*args, *more)


def feed_back_kernel(n2_ref, go_ref, gt_ref, gp_ref, s1_ref, x_ref, y_ref, st_ref, gain_ref, we_ref, ws_ref, *refs, count, last, fsdp):
    s_refs = refs[: 1 + last]
    send_ref, keep_ref, cols_ref, bias_ref, acc = refs[1 + last :]

    @at_first()
    def _():
        acc[...] = jnp.zeros_like(acc)
        cols_ref[...] = jnp.zeros_like(cols_ref)
        bias_ref[...] = jnp.zeros_like(bias_ref)

    n2, g = n2_ref[...], pick((go_ref, gt_ref), count)
    pre_grad = (dot(g, ws_ref[...]) * gp_ref[...].astype(f32)).astype(bf16)
    bias_ref[...] += jnp.sum(pre_grad.astype(f32), axis=0, keepdims=True)
    s = dot(pre_grad, we_ref[...], 1, 1)
    acc[...] += dot(n2, pre_grad, 0, 0)
    normal = normal_of((x_ref, y_ref), st_ref, count)
    cols_ref[0:1, :] += jnp.sum(s * normal, axis=0, keepdims=True)
    cols_ref[1:2, :] += jnp.sum(s, axis=0, keepdims=True)
    s = s1_ref[...] + s * gain_ref[...]
    if last:
        put(s_refs, count, s.astype(bf16))
    else:
        s_refs[0][...] = s

    @at_last()
    def _():
        put_blocks(fsdp, (send_ref, keep_ref), acc)


def feed_back_call(fsdp, n2, grads, gp, s1, x, st, vec, w2, half, last, rows=256):
    g, d = n2.shape
    hidden = gp.shape[1] // 2
    own = x[0].shape[0]
    n, count = g // rows, own // rows
    return call(
        functools.partial(feed_back_kernel, count=count, last=last, fsdp=fsdp),
        (n,),
        [own_order(rows, d)]
        + both(rows, d, count)
        + [pl.BlockSpec((rows, hidden), lambda i, *s: (i, half)), own_order(rows, d)]
        + both(rows, d, count)
        + [own_order(rows, 2), held(1, d), weight_of(w2, 0, half), weight_of(w2, 1, half)],
        (both(rows, d, count) if last else [own_order(rows, d)]) + [pieces(d, hidden)[0]] * 2 + [held(2, d), held(1, hidden)],
        ([shape(own, d, bf16), shape(g - own, d, bf16)] if last else [shape(g, d, f32)])
        + [pieces(d, hidden)[1]] * 2
        + [shape(2, d, f32), shape(1, hidden, f32)],
        [pltpu.VMEM((d, hidden), f32)],
        6 * g * d * hidden,
        0,
    )(n2, *grads, gp, s1, *x, st, vec[2], w2, w2)


TAIL = 7
LAST_PIECES = 4


def feed_back_last_kernel(
    n2_ref, go_ref, gt_ref, gp_ref, s1_ref, x_ref, y_ref, st_ref, gain_ref, we_ref, ws_ref, d_send, d_keep, cols_ref, bias_ref, late_hbm, late_own_ref,
    grad_ref, dws_ref, dwe_ref, sum_ref, out_ref,
    late_got, acc, to_owner, from_other, own_s, e_send, parts, parts_got, *scratch, count,
):
    n = 2 * count
    d = acc.shape[0]
    step = pl.program_id(0)
    to = neighbours()
    row_sems, sum_sems, late_sems, scratch = scratch[0:2], scratch[2:4], scratch[4:6], scratch[6:]
    size = len(scratch) // 2
    shrink = Reduce(d_send, kept(d_keep, d), dws_ref, scratch[:size], to)

    def from_acc(p, j):
        rows = d // 16
        return acc[pl.ds(pl.multiple_of(block_order(j) * rows, rows), rows), expand.cols(p)]

    expand = Reduce(e_send, lambda p, j: from_acc(p, 8 + j), dwe_ref, scratch[size:], to)
    small = SumAll(parts, parts_got, sum_sems, to)
    row_copy = lambda b: remote(to_owner.at[b], from_other.at[b], row_sems, b, to["y"])
    late_copy = remote(late_hbm, late_got, late_sems, 0, to["y"])
    normal = (jnp.where(step < count, y_ref[...], x_ref[...]).astype(f32) - st_ref[:, 0:1]) * st_ref[:, 1:2]

    @at_step(0)
    def _():
        acc[...] = jnp.zeros_like(acc)
        parts[0] = jnp.zeros_like(sum_ref)
        parts[0, 0:2, :] = cols_ref[...]
        wide = bias_ref.shape[1]
        for r in range(3):
            at = r * wide % d
            parts[0, 5 + r * wide // d : 6 + r * wide // d, at : at + wide] = bias_ref[r : r + 1, :]
        greet(to)
        late_copy.start()
        for p in range(PIECES):
            shrink.across_core(p)

    @at_step(1)
    def _():
        for p in range(PIECES):
            shrink.across_x(p)

    for p, at in enumerate((4, 6)):
        pl.when(step == at)(functools.partial(shrink.along_z, p))
    for b in range(count):

        @at_step(b + 1)
        def _():
            row_copy(b).start()

    @pl.when(step < n)
    def _():
        own = step >= count
        n2, g = n2_ref[...], jnp.where(own, go_ref[...], gt_ref[...])
        pre_grad = (dot(g, ws_ref[...]) * gp_ref[...].astype(f32)).astype(bf16)
        bias = jnp.sum(pre_grad.astype(f32), axis=0, keepdims=True)
        for r in range(pre_grad.shape[1] // d):
            parts[0, 7 + r : 8 + r, :] += bias[:, r * d : (r + 1) * d]
        s = dot(pre_grad, we_ref[...], 1, 1)
        acc[...] += dot(n2, pre_grad, 0, 0)
        parts[0, 2:3, :] += jnp.sum(s * normal, axis=0, keepdims=True)
        parts[0, 3:4, :] += jnp.sum(s, axis=0, keepdims=True)
        s = s1_ref[...] + s * gain_ref[...]

        @pl.when(own)
        def _():
            own_s[step - count] = s
            parts[0, 4:5, :] += jnp.sum(g.astype(f32), axis=0, keepdims=True)

        @pl.when(jnp.logical_not(own))
        def _():
            to_owner[step] = s.astype(bf16)

    @at_step(n)
    def _():
        small.start(0)
        for p in range(LAST_PIECES):
            for j in range(8):
                e_send[p, expand.block(j)] = from_acc(p, j).astype(bf16)
        for p in range(LAST_PIECES):
            expand.across_core(p)

    @at_step(n + 1)
    def _():
        small.turn(0)
        for p in range(LAST_PIECES):
            expand.across_x(p)

    for p in range(LAST_PIECES):

        @at_step(n + 2 + p)
        def _():
            if p < 3:
                small.turn(p + 1)
            else:
                sum_ref[...] = small.end(5)
            expand.along_z(p)

    @at_step(n + 2)
    def _():
        for p in range(PIECES):
            shrink.end(p)

    for b in range(count):

        @at_step(n + b)
        def _():
            row_copy(b).wait()
            s = own_s[b] + from_other[b].astype(f32)
            centred = s - jnp.mean(s, axis=1, keepdims=True) - normal * jnp.mean(s * normal, axis=1, keepdims=True)
            grad_ref[...] = go_ref[...].astype(f32) + st_ref[:, 1:2] * centred

    @at_step(n)
    def _():
        late_copy.wait()
        out_ref[...] = (late_own_ref[...] + late_got[...].astype(f32)).astype(bf16)

    @at_step(n + TAIL - 1)
    def _():
        for p in range(LAST_PIECES):
            expand.end(p)


def feed_back_last_call(n2, grads, gp, s1, x, st, vec, w2, dws, cols, bias, late, rows=256):
    g, d = n2.shape
    hidden = gp.shape[1]
    own = x[0].shape[0]
    n, count = g // rows, own // rows
    part = d // 16
    first = lambda c: pl.BlockSpec((rows, c), lambda i: (jnp.minimum(i, count - 1), 0))
    second = lambda c: pl.BlockSpec((rows, c), lambda i: (jnp.where(i < n, jnp.maximum(i - count, 0), jnp.minimum(i - n, count - 1)), 0))
    turned = lambda c: pl.BlockSpec((rows, c), lambda i: (jnp.where(i < n, lax.rem(i + count, n), jnp.minimum(i - n, count - 1)), 0))
    turned_once = lambda c: pl.BlockSpec((rows, c), lambda i: (lax.rem(jnp.minimum(i, n - 1) + count, n), 0))
    ins = [turned_once(d), second(d), first(d), turned_once(hidden), turned_once(d), second(d), first(d), turned(2), held(1, d)]
    ins += [weight_of(w2, 0), weight_of(w2, 1), pl.BlockSpec(memory_space=pl.ANY), pieces(d, hidden)[0], held(2, d), held(*bias.shape)]
    ins += [pl.BlockSpec(memory_space=pl.ANY), held(rows, d)]
    small = jax.ShapeDtypeStruct((16, d), f32)
    outs = [pl.BlockSpec((rows, d), lambda i: (jnp.clip(i - n, 0, count - 1), 0)), held(part, hidden), held(part, hidden), held(*small.shape), held(rows, d)]
    shapes = [shape(own, d, f32), shape(part, hidden, f32), shape(part, hidden, f32), shape(*small.shape, f32), shape(rows, d, bf16)]
    rows_buffer = lambda dtype: pltpu.VMEM((count, rows, d), dtype)
    sums = pltpu.VMEM((5, *small.shape), f32)
    scratch = [pltpu.VMEM((rows, d), bf16), pltpu.VMEM((d, hidden), f32), rows_buffer(bf16), rows_buffer(bf16), rows_buffer(f32)]
    scratch += [pltpu.VMEM((LAST_PIECES, d // 2, hidden // LAST_PIECES), bf16), sums, sums]
    scratch += sem_pair(count) + sem_pair(5) + sem_pair(1) + Reduce.scratch(d, hidden) + Reduce.scratch(d, hidden, LAST_PIECES)
    return call(functools.partial(feed_back_last_kernel, count=count), (n + TAIL,), ins, outs, shapes, scratch, 6 * g * d * hidden, 0, collective=1)(
        n2, *grads, gp, s1, *x, st, vec[2], w2, w2, *dws, cols, bias, *late
    )


def rotary_tables():
    half = ROT // 2
    position = jnp.arange(LEN).astype(f32)
    inverse = 10000.0 ** (-(jnp.arange(half).astype(f32) * 2.0) / ROT)
    angle = position[:, None] * inverse[None, :]
    cos, sin = jnp.cos(angle), jnp.sin(angle)
    rest = jnp.zeros((LEN, HS - ROT), f32)
    none = jnp.zeros((LEN, half), f32)
    period = lambda *a: jnp.tile(jnp.concatenate(a, axis=1), (1, 128 // HS))
    return period(cos, cos, rest + 1.0), period(-sin, none, rest), period(none, sin, rest)


def join(a):
    return jnp.concatenate(list(a), axis=1)


def make_body(fsdp, tp):
    fast = (fsdp, tp) == (16, 2)

    def body(inputs, cotangent, first_gain, first_shift, second_gain, second_shift, project_weight, project_bias, dense_weight, dense_bias, expand_weight, expand_bias, shrink_weight, shrink_bias):
        rows, d = inputs.shape
        width = dense_weight.shape[0]
        hidden = shrink_weight.shape[0]
        part = project_weight.shape[0]
        me = lax.axis_index("tp")
        split = lambda a: (a[:rows], a[rows:])
        zero = jnp.zeros((1,), jnp.int32)
        vec = [a[None] for a in (first_gain, first_shift, second_gain, second_shift)]
        if fast:
            shift = (me * rows).astype(jnp.int32)[None]
            n1, n2, st, ctx, dq, dk, dv, w1, x, grads, w2 = head_call(
                inputs, cotangent, project_weight.transpose(1, 0, 2), dense_weight.T, expand_weight, shrink_weight.T, vec, project_bias
            )
            w2 = w2.reshape(2, d, hidden)
            x, grads = (inputs, x), (cotangent, grads)
        else:
            shift = zero
            gather = lambda a: lax.all_gather(a, "fsdp", axis=0, tiled=True)
            w1 = gather(jnp.concatenate([project_weight.reshape(part, 3 * width), dense_weight.T], axis=1))
            w2 = jnp.stack([gather(expand_weight), gather(shrink_weight.T)])
            tables = rotary_tables()
            x = split(lax.all_gather(inputs, "tp", axis=0, tiled=True))
            grads = split(lax.all_gather(cotangent, "tp", axis=0, tiled=True))
            n1, n2, st, q, k, v = qkv_call(shift, x, vec, w1, project_bias, tables, width)
            do = context_grad_call(zero, jnp.concatenate(grads), w1, width)
            ctx, dq, dk, dv = attention_call(q, k, v, do, tables)
        s, *dw1, cols1, bias1 = project_back_call(shift, fsdp, dq, dk, dv, ctx, n1, x, st, grads, vec, w1)
        out_bias = dense_bias + shrink_bias
        if fast:
            gp, output, *late, send, keep, dw1 = feed_forward_call(fsdp, n2, grads, ctx, w2, w1, expand_bias[None], (inputs, out_bias[None], *dw1))
        else:
            gp, *branch = feed_forward_call(fsdp, n2, grads, ctx, w2, w1, expand_bias[None])
            branch, dws = branch[:2], branch[2:]
        if fast:
            input_grad, dws, dwe, small, rest = feed_back_last_call(n2, grads, gp, s, x, st, vec, w2, (send, keep), cols1, bias1, late)
            output = jnp.concatenate([output, rest])
            cols, local = small[:5], jnp.concatenate([small[5:7].reshape(-1)[: 3 * width], small[7:9].reshape(-1)])
        else:
            s, *dwe, cols2, bias2 = feed_back_call(fsdp, n2, grads, gp, s, x, st, vec, w2, 0, False)
            *s, send, keep, cols3, bias3 = feed_back_call(fsdp, n2, grads, gp, s, x, st, vec, w2, 1, True)
            over = lambda a, axis: lax.psum_scatter(jnp.concatenate(a), axis, scatter_dimension=0, tiled=True).astype(f32)
            scatter = lambda pair: over([join(a) for a in pair], "fsdp")
            s = over(s, "tp")
            own_rows = inputs.astype(f32)
            output = (own_rows + over(branch, "tp") + out_bias).astype(bf16)
            own_st = lax.dynamic_slice_in_dim(st, me * rows, rows, 0)
            own_bias = jnp.sum(cotangent.astype(f32), axis=0, keepdims=True)
            cols = lax.psum(jnp.concatenate([cols1, cols2 + cols3, own_bias]), ("fsdp", "tp"))
            local = lax.psum(jnp.concatenate([bias1.reshape(-1), bias2.reshape(-1), bias3.reshape(-1)]), "fsdp")
            dw1 = scatter(dw1).reshape(part, 4, width).transpose(1, 0, 2)
            dws, dwe = scatter(dws), jnp.concatenate([scatter(dwe), scatter((send, keep))], axis=1)
            normal = (own_rows - own_st[:, 0:1]) * own_st[:, 1:2]
            term = own_st[:, 1:2] * (s - jnp.mean(s, axis=1, keepdims=True) - normal * jnp.mean(s * normal, axis=1, keepdims=True))
            input_grad = cotangent.astype(f32) + term
        return (
            output,
            input_grad,
            cols[0],
            cols[1],
            cols[2],
            cols[3],
            dw1[:3].transpose(1, 0, 2),
            local[: 3 * width].reshape(3, width),
            dw1[3].T,
            cols[4],
            dwe,
            local[3 * width :],
            dws.T,
            cols[4],
        )

    return body


def solution(mesh):
    rows, rep = P(("fsdp", "tp"), None), P()
    return jax.shard_map(
        make_body(mesh.shape["fsdp"], mesh.shape["tp"]),
        mesh=mesh,
        in_specs=(rows, rows, rep, rep, rep, rep, P("fsdp", None, "tp"), P(None, "tp"), P("tp", "fsdp"), rep, P("fsdp", "tp"), P("tp"), P("tp", "fsdp"), rep),
        out_specs=(rows, rows, rep, rep, rep, rep, P("fsdp", None, "tp"), P(None, "tp"), P("tp", "fsdp"), rep, P("fsdp", "tp"), P("tp"), P("tp", "fsdp"), rep),
        check_vma=False,
    )
```
